32 devices in a mesh: data: 1 (over z), fsdp: 32 (over y, x, core).
Axes of the slice: x: 4, y: 4, z: 1, core: 2. Of those that a mesh axis runs over, the one named last changes fastest.
The devices are a block of a 4x4x8 slice.
Arguments:
- hidden: bfloat16 [16384, 2048], P('data')
- targets: int32 [16384], P('data')
- w_out: bfloat16 [49152, 2048], P('fsdp')
Outputs:
- output 1: float32 [1], P('data')
- output 2: float32 [16384, 2048], P(('data', 'fsdp'))
- output 3: float32 [49152, 2048], P(('data', 'fsdp'))
All inputs are finite; a program needn't handle non-finite values.
Results may differ from the reference program's by a relative error of at most 0.001.
Values are sent between devices in bfloat16 or wider.
A program may use at most 768 MiB of HBM per device.

```python
import math
import jax
import jax.numpy as jnp
from jax import lax

GROUP_SIZE = 32
TOKENS_DEV = 512
VOCAB_SIZE = 49152
MODEL_DIM = 2048

TOKENS = TOKENS_DEV * GROUP_SIZE
VOCAB_DEV = VOCAB_SIZE // GROUP_SIZE


def setup_inputs(seed: int = 0, part: int = 0) -> dict:
    base_key = jax.random.key(seed)
    shared_key, part_base = jax.random.split(base_key)
    part_key = jax.random.fold_in(part_base, part)
    noise_key, offset_key, perm_key = jax.random.split(part_key, 3)
    w_out = (jax.random.normal(shared_key, (VOCAB_SIZE, MODEL_DIM), jnp.float32) * MODEL_DIM ** -0.5).astype(jnp.bfloat16)
    positions = jnp.arange(TOKENS)
    offsets = jax.random.randint(offset_key, (TOKENS,), 0, VOCAB_DEV)
    offsets = jnp.where(positions == 0, 0, offsets)
    offsets = jnp.where(positions == GROUP_SIZE - 1, VOCAB_DEV - 1, offsets)
    targets = jax.random.permutation(perm_key, (positions % GROUP_SIZE) * VOCAB_DEV + offsets).astype(jnp.int32)
    boost = math.log(VOCAB_SIZE)
    hidden = jax.random.normal(noise_key, (TOKENS, MODEL_DIM), jnp.float32) + boost * w_out.astype(jnp.float32)[targets]
    return {"hidden": hidden.astype(jnp.bfloat16), "targets": targets, "w_out": w_out}


def reference(hidden, targets, w_out):
    hid_blocks = hidden.reshape(GROUP_SIZE, TOKENS_DEV, MODEL_DIM)
    tgt_blocks = targets.reshape(GROUP_SIZE, TOKENS_DEV)
    vocab_ids = jnp.arange(VOCAB_SIZE)[None, :]

    def scan_step(grad_w, blocks):
        hid_blk, tgt_blk = blocks
        logits = jnp.dot(hid_blk, w_out.T, preferred_element_type=jnp.float32)
        row_max = jnp.max(logits, axis=1, keepdims=True)
        log_norm = row_max + jnp.log(jnp.sum(jnp.exp(logits - row_max), axis=1, keepdims=True))
        tgt_hit = vocab_ids == tgt_blk[:, None]
        tgt_logit = jnp.sum(jnp.where(tgt_hit, logits, 0.0), axis=1, keepdims=True)
        probs = jnp.exp(logits - log_norm)
        grad_logits = ((probs - tgt_hit.astype(jnp.float32)) / TOKENS).astype(jnp.bfloat16)
        grad_hid = jnp.dot(grad_logits, w_out, preferred_element_type=jnp.float32)
        grad_w = grad_w + jnp.dot(grad_logits.T, hid_blk, preferred_element_type=jnp.float32)
        return grad_w, (jnp.sum(log_norm - tgt_logit), grad_hid)

    grad_w, (loss_terms, grad_hid) = lax.scan(scan_step, jnp.zeros((VOCAB_SIZE, MODEL_DIM), jnp.float32), (hid_blocks, tgt_blocks))
    loss_val = (jnp.sum(loss_terms) / TOKENS).reshape(1)
    return loss_val, grad_hid.reshape(TOKENS, MODEL_DIM), grad_w
```

```python
import functools
import math

import jax
import jax.numpy as jnp
from jax import lax
from jax.experimental import pallas as pl
from jax.experimental.pallas import tpu as pltpu
from jax.sharding import PartitionSpec as P

F32 = jnp.float32
BF16 = jnp.bfloat16
LOG2E = 1.4426950408889634
LN2 = 0.6931471805599453
ROWS = 16
AXIS = "fsdp"

FAR1, PURE1, MERGED1, FAR2, PURE2, MERGED2 = range(6)


def dot_nt(a, b):
    return lax.dot_general(a, b, (((1,), (1,)), ((), ())), preferred_element_type=F32)


def dot_nn(a, b):
    return lax.dot_general(a, b, (((1,), (0,)), ((), ())), preferred_element_type=F32)


def dot_tn(a, b):
    return lax.dot_general(a, b, (((0,), (0,)), ((), ())), preferred_element_type=F32)


def join(parts):
    top = functools.reduce(jnp.maximum, parts)
    total = functools.reduce(jnp.add, [jnp.exp2(v - top) for v in parts])
    return top + jnp.log(total) * LOG2E


def head_kernel(
    group, side, chunks, tokens,
    hid, tgt, w_hbm,
    loss_ref, dh_hbm, dw_hbm,
    wb, dwacc, hb, yb, yt, dz, dzr, sb, tb, far1, pure1, merged1, far2, pure2, merged2, ob,
    stat, own, st0, mid, st1, row, st2, lse, lossacc,
    wsem, hsem, rs_send, rs_recv, dz_send, dz_recv, w_send, w_recv,
    st0_send, st0_recv, st1_send, st1_recv, st2_send, st2_recv, osem, dwsem,
):
    vocab, dim = w_hbm.shape
    half = dim // 2
    mt = vocab // 2
    tok = hb.shape[1] * hb.shape[2] * ROWS
    tokc = tok // 2

    me = lax.axis_index(AXIS)
    core = lax.rem(me, 2)
    other = 1 - core
    x = lax.rem(me // 2, side)
    y = me // (2 * side)
    p = x + core * (y - x)
    q = y + core * (x - y)
    partner = me + 1 - 2 * core

    def at_xy(xx, yy):
        return (lax.rem(yy + side, side) * side + lax.rem(xx + side, side)) * 2 + core

    def at_pq(pp, qq):
        return at_xy(pp + core * (qq - pp), qq + core * (pp - qq))

    def rcopy(src, dst, send, recv, dev):
        return pltpu.make_async_remote_copy(
            src_ref=src, dst_ref=dst, send_sem=send, recv_sem=recv,
            device_id={AXIS: dev}, device_id_type=pl.DeviceIdType.MESH,
        )

    def guarded(cond, fn):
        pl.when(cond)(fn)

    barrier = pltpu.get_barrier_semaphore()
    friends = [partner] + [at_xy(x + k, y) for k in range(1, side)] + [at_xy(x, y + k) for k in range(1, side)]
    for dev in friends:
        pl.semaphore_signal(barrier, inc=1, device_id={AXIS: dev}, device_id_type=pl.DeviceIdType.MESH)

    def h_copies(c):
        s = lax.rem(c, 4)
        out = []
        for k in range(side):
            out.append(pltpu.make_async_copy(hid.at[:, k, 0, c], hb.at[s, k], hsem.at[s]))
            out.append(pltpu.make_async_copy(hid.at[k, :, 1, c], hb.at[s, side + k], hsem.at[s]))
        return out

    def h_start(c):
        for d in h_copies(c):
            d.start()

    def h_wait(c):
        s = lax.rem(c, 4)
        pltpu.make_async_copy(hb.at[s], hb.at[s], hsem.at[s]).wait()

    w_local = pltpu.make_async_copy(w_hbm, wb.at[core], wsem)
    w_local.start()
    h_start(0)
    dwacc[...] = jnp.zeros_like(dwacc)
    lossacc[...] = jnp.zeros_like(lossacc)
    pl.semaphore_wait(barrier, len(friends))
    w_local.wait()
    w_remote = rcopy(wb.at[core], wb.at[core], w_send, w_recv, partner)
    w_remote.start()

    def rs(kind, c):
        s = lax.rem(c, 2)
        lo, hi = pl.ds(0, half), pl.ds(half, half)
        if kind in (FAR1, PURE1, MERGED1):
            a, buf = p, sb
            to = (at_pq(p + 1, q), at_pq(p - 1, q))
        else:
            a, buf = q, tb
            to = (at_pq(p, q + 1), at_pq(p, q - 1))
        up, down, far = lax.rem(a + 1, side), lax.rem(a + side - 1, side), lax.rem(a + 2, side)
        dst = (far1, pure1, merged1, far2, pure2, merged2)[kind]
        src = {0: ((far, lo), (far, hi)), 1: ((up, hi), (down, lo)), 2: ((up, lo), (down, hi))}[kind % 3]
        return [
            rcopy(buf.at[s, src[d][0], :, src[d][1]], dst.at[s, d], rs_send.at[kind, s, d], rs_recv.at[kind, s, d], to[d])
            for d in range(2)
        ]

    def start(ds):
        for d in ds:
            d.start()

    def wait_recv(ds):
        for d in ds:
            d.wait_recv()

    def wait_send(ds):
        for d in ds:
            d.wait_send()

    def dz_copy(c):
        s = lax.rem(c, 2)
        return [rcopy(dz.at[other], dzr.at[s], dz_send, dz_recv.at[s], partner)]

    def st0_copy(i):
        s = lax.rem(i, 2)
        return [rcopy(own.at[s], st0.at[s], st0_send.at[s], st0_recv.at[s], partner)]

    def st1_copy(i):
        s = lax.rem(i, 2)
        return [
            rcopy(mid.at[s], st1.at[s, x], st1_send.at[s, k - 1], st1_recv.at[s, k - 1], at_xy(x + k, y))
            for k in range(1, side)
        ]

    def st2_copy(i):
        s = lax.rem(i, 2)
        return [
            rcopy(row.at[s], st2.at[s, y], st2_send.at[s, k - 1], st2_recv.at[s, k - 1], at_xy(x, y + k))
            for k in range(1, side)
        ]

    def logits(i, j):
        r = pl.ds(j * mt, mt)
        h = hb[lax.rem(i, 4)].reshape(tok, dim)
        v = dot_nt(wb[core, r, :], h) * LOG2E
        yb[lax.rem(i, 2), r, :] = v
        yt[...] = v

    def grad_logits(c, j):
        r = pl.ds(j * mt, mt)
        prob = jnp.exp2(yb[lax.rem(c, 2), r, :] - lse[0:1, :])
        rel = tgt[c] - (me * vocab + j * mt)
        hit = lax.broadcasted_iota(jnp.int32, prob.shape, 0) == rel
        g = (prob + jnp.where(hit, -1.0 / tokens, 0.0)).astype(BF16)
        dz[0, r, :] = g[:, :tokc]
        dz[1, r, :] = g[:, tokc:]

    def statistics(i, j):
        v = yt[...]
        top = jnp.max(v, axis=0, keepdims=True)
        total = jnp.sum(jnp.exp2(v - top), axis=0, keepdims=True)
        rel = tgt[i] - (me * vocab + j * mt)
        hit = lax.broadcasted_iota(jnp.int32, v.shape, 0) == rel
        stat[j, 0:1, :] = top + jnp.log(total) * LOG2E
        stat[j, 1:2, :] = jnp.sum(jnp.where(hit, v, 0.0), axis=0, keepdims=True)

    def grad_w(c):
        s = lax.rem(c, 4)
        n = dim // 2

        def body(k, carry):
            cols = pl.ds(pl.multiple_of(k * n, n), n)
            h = hb[s, :, :, :, cols].reshape(tok, n)
            dwacc[:, cols] += dot_nn(dz[0], h[:tokc]) + dot_nn(dz[1], h[tokc:])
            return carry

        lax.fori_loop(0, dim // n, body, 0)

    def grad_h(c):
        s = lax.rem(c, 2)
        n = dim // 2

        def body(k, carry):
            cols = pl.ds(pl.multiple_of(k * n, n), n)
            v = dot_tn(dz[core], wb[core, :, cols]) + dot_tn(dzr[s], wb[other, :, cols])
            sb[s, :, :, cols] = v.reshape(side, side * ROWS, n)
            return carry

        lax.fori_loop(0, dim // n, body, 0)

    def finish(c):
        s = lax.rem(c, 2)
        wait_recv(rs(PURE2, c) + rs(MERGED2, c))
        wait_send(rs(FAR2, c) + rs(PURE2, c) + rs(MERGED2, c))
        guarded(c >= 2, lambda: pltpu.make_async_copy(ob.at[s], dh_hbm.at[c - 2], osem.at[s]).wait())
        ob[s, :, :half] = tb[s, q, :, :half] + merged2[s, 0] + pure2[s, 1]
        ob[s, :, half:] = tb[s, q, :, half:] + pure2[s, 0] + merged2[s, 1]
        pltpu.make_async_copy(ob.at[s], dh_hbm.at[c], osem.at[s]).start()

    def turn(c):
        s = lax.rem(c, 2)
        wait_recv(rs(PURE1, c) + rs(MERGED1, c))
        lo = sb[s, p, :, :half] + merged1[s, 0] + pure1[s, 1]
        hi = sb[s, p, :, half:] + pure1[s, 0] + merged1[s, 1]
        tb[s, :, :, :half] = lo.reshape(side, ROWS, half)
        tb[s, :, :, half:] = hi.reshape(side, ROWS, half)
        start(rs(FAR2, c) + rs(PURE2, c))
        wait_send(rs(FAR1, c) + rs(PURE1, c) + rs(MERGED1, c))

    def merge1(c):
        s = lax.rem(c, 2)
        up, down = lax.rem(p + 1, side), lax.rem(p + side - 1, side)
        wait_recv(rs(FAR1, c))
        sb[s, up, :, :half] += far1[s, 0]
        sb[s, down, :, half:] += far1[s, 1]
        start(rs(MERGED1, c))

    def merge2(c):
        s = lax.rem(c, 2)
        up, down = lax.rem(q + 1, side), lax.rem(q + side - 1, side)
        wait_recv(rs(FAR2, c))
        tb[s, up, :, :half] += far2[s, 0]
        tb[s, down, :, half:] += far2[s, 1]
        start(rs(MERGED2, c))

    def st_own(i):
        s = lax.rem(i, 2)
        guarded(i >= 2, lambda: wait_send(st0_copy(i)))
        own[s, 0:1, :] = join([stat[0, 0:1, :], stat[1, 0:1, :]])
        own[s, 1:2, :] = stat[0, 1:2, :] + stat[1, 1:2, :]
        start(st0_copy(i))

    def st_pair(i):
        s = lax.rem(i, 2)
        wait_recv(st0_copy(i))
        guarded(i >= 2, lambda: wait_send(st1_copy(i)))
        mid[s, 0:1, :] = join([own[s, 0:1, :], st0[s, 0:1, :]])
        mid[s, 1:2, :] = own[s, 1:2, :] + st0[s, 1:2, :]
        st1[s, x] = mid[s]
        start(st1_copy(i))

    def st_row(i):
        s = lax.rem(i, 2)
        wait_recv(st1_copy(i))
        guarded(i >= 2, lambda: wait_send(st2_copy(i)))
        row[s, 0:1, :] = join([st1[s, k, 0:1, :] for k in range(side)])
        row[s, 1:2, :] = functools.reduce(jnp.add, [st1[s, k, 1:2, :] for k in range(side)])
        st2[s, y] = row[s]
        start(st2_copy(i))

    def st_all(i):
        s = lax.rem(i, 2)
        wait_recv(st2_copy(i))
        full = join([st2[s, k, 0:1, :] for k in range(side)])
        hit = functools.reduce(jnp.add, [st2[s, k, 1:2, :] for k in range(side)])
        lse[0:1, :] = full + math.log2(tokens)
        lossacc[...] += full - hit

    def step(i, carry):
        c = i - 2
        has_a, has_c = i < chunks, jnp.logical_and(c >= 0, c < chunks)

        @pl.when(i + 1 < chunks)
        def _():
            h_start(i + 1)

        @pl.when(has_a)
        def _():
            h_wait(i)

        @pl.when(jnp.logical_and(has_a, has_c))
        def _():
            grad_logits(c, 0)
            logits(i, 0)

        @pl.when(jnp.logical_and(has_a, has_c))
        def _():
            grad_logits(c, 1)
            statistics(i, 0)
            logits(i, 1)

        @pl.when(jnp.logical_and(has_a, jnp.logical_not(has_c)))
        def _():
            logits(i, 0)
            statistics(i, 0)
            logits(i, 1)

        @pl.when(jnp.logical_and(has_c, jnp.logical_not(has_a)))
        def _():
            grad_logits(c, 0)
            grad_logits(c, 1)

        @pl.when(has_c)
        def _():
            start(dz_copy(c))

        @pl.when(has_a)
        def _():
            statistics(i, 1)
            st_own(i)

        def live(k):
            return jnp.logical_and(k >= 0, k < chunks)

        guarded(live(c - 3), lambda: finish(c - 3))
        guarded(live(c - 2), lambda: turn(c - 2))
        guarded(live(c - 1), lambda: start(rs(PURE1, c - 1)))
        guarded(live(i - 1), lambda: st_row(i - 1))

        @pl.when(has_c)
        def _():
            grad_w(c)

        guarded(live(c - 1), lambda: merge1(c - 1))
        guarded(live(c - 2), lambda: merge2(c - 2))
        guarded(has_a, lambda: st_pair(i))

        @pl.when(has_c)
        def _():
            guarded(c == 0, w_remote.wait_recv)
            wait_recv(dz_copy(c))
            grad_h(c)
            start(rs(FAR1, c))
            wait_send(dz_copy(c))

        guarded(live(i - 1), lambda: st_all(i - 1))

        @pl.when(c == chunks - 1)
        def _():
            pltpu.make_async_copy(dwacc, dw_hbm, dwsem).start()

        return carry

    lax.fori_loop(0, chunks + 5, step, 0)

    for i in range(max(chunks - 2, 0), chunks):
        wait_send(st0_copy(i) + st1_copy(i) + st2_copy(i))
        pltpu.make_async_copy(ob.at[i % 2], dh_hbm.at[i], osem.at[i % 2]).wait()
    w_remote.wait_send()
    pltpu.make_async_copy(dwacc, dw_hbm, dwsem).wait()
    loss_ref[...] = jnp.broadcast_to(jnp.sum(lossacc[...], axis=1, keepdims=True) * (LN2 / tokens), loss_ref.shape)


def solution(mesh):
    group = mesh.shape[AXIS]
    side = math.isqrt(group // 2)

    def local_step(hidden, targets, w_blk):
        tokens, dim = hidden.shape
        vocab = w_blk.shape[0]
        chunks = tokens // group // ROWS
        tok = group * ROWS
        half = dim // 2
        hid = hidden.reshape(side, side, 2, chunks, ROWS, dim)
        t = targets.reshape(side, side, 2, chunks, ROWS)
        tgt = jnp.concatenate(
            [t[:, :, 0].transpose(2, 1, 0, 3).reshape(chunks, 1, tok // 2), t[:, :, 1].transpose(2, 0, 1, 3).reshape(chunks, 1, tok // 2)],
            axis=2,
        )
        dma = pltpu.SemaphoreType.DMA
        any_spec = pl.BlockSpec(memory_space=pl.ANY)
        vmem_spec = pl.BlockSpec(memory_space=pltpu.VMEM)
        big, small = (2, 2, side * ROWS, half), (2, 2, ROWS, half)
        loss, dh, dw = pl.pallas_call(
            functools.partial(head_kernel, group, side, chunks, tokens),
            out_shape=(
                jax.ShapeDtypeStruct((1, 128), F32),
                jax.ShapeDtypeStruct((chunks, ROWS, dim), F32),
                jax.ShapeDtypeStruct((vocab, dim), F32),
            ),
            in_specs=[any_spec, vmem_spec, any_spec],
            out_specs=(vmem_spec, any_spec, any_spec),
            scratch_shapes=[
                pltpu.VMEM((2, vocab, dim), BF16),
                pltpu.VMEM((vocab, dim), F32),
                pltpu.VMEM((4, 2 * side, side, ROWS, dim), BF16),
                pltpu.VMEM((2, vocab, tok), F32),
                pltpu.VMEM((vocab // 2, tok), F32),
                pltpu.VMEM((2, vocab, tok // 2), BF16),
                pltpu.VMEM((2, vocab, tok // 2), BF16),
                pltpu.VMEM((2, side, side * ROWS, dim), F32),
                pltpu.VMEM((2, side, ROWS, dim), F32),
                *[pltpu.VMEM(big, F32)] * 3,
                *[pltpu.VMEM(small, F32)] * 3,
                pltpu.VMEM((2, ROWS, dim), F32),
                pltpu.VMEM((2, 2, tok), F32),
                pltpu.VMEM((2, 2, tok), F32),
                pltpu.VMEM((2, 2, tok), F32),
                pltpu.VMEM((2, 2, tok), F32),
                pltpu.VMEM((2, side, 2, tok), F32),
                pltpu.VMEM((2, 2, tok), F32),
                pltpu.VMEM((2, side, 2, tok), F32),
                pltpu.VMEM((1, tok), F32),
                pltpu.VMEM((1, tok), F32),
                dma, dma((4,)),
                dma((6, 2, 2)), dma((6, 2, 2)),
                dma, dma((2,)), dma, dma,
                dma((2,)), dma((2,)),
                dma((2, side - 1)), dma((2, side - 1)),
                dma((2, side - 1)), dma((2, side - 1)),
                dma((2,)), dma,
            ],
            compiler_params=pltpu.CompilerParams(
                collective_id=0, has_side_effects=True, vmem_limit_bytes=67043328,
            ),
            name="head",
        )(hid, tgt, w_blk)
        return loss[0, :1], dh.reshape(tokens // group, dim), dw

    return jax.shard_map(
        local_step,
        mesh=mesh,
        in_specs=(P("data", None), P("data"), P(AXIS, None)),
        out_specs=(P("data"), P(("data", AXIS), None), P(("data", AXIS), None)),
        check_vma=False,
    )
```

```python
import functools
import math

import jax
import jax.numpy as jnp
from jax import lax
from jax.experimental import pallas as pl
from jax.experimental.pallas import tpu as pltpu
from jax.sharding import PartitionSpec as P

F32 = jnp.float32
BF16 = jnp.bfloat16
LOG2E = 1.4426950408889634
LN2 = 0.6931471805599453
ROWS = 16
AXIS = "fsdp"

FAR1, PURE1, MERGED1, FAR2, PURE2, MERGED2 = range(6)


def dot_nt(a, b):
    return lax.dot_general(a, b, (((1,), (1,)), ((), ())), preferred_element_type=F32)


def dot_nn(a, b):
    return lax.dot_general(a, b, (((1,), (0,)), ((), ())), preferred_element_type=F32)


def dot_tn(a, b):
    return lax.dot_general(a, b, (((0,), (0,)), ((), ())), preferred_element_type=F32)


def join(parts):
    top = functools.reduce(jnp.maximum, parts)
    total = functools.reduce(jnp.add, [jnp.exp2(v - top) for v in parts])
    return top + jnp.log(total) * LOG2E


def head_kernel(
    group, side, chunks, tokens,
    hid, tgt, w_hbm,
    loss_ref, dh_hbm, dw_hbm,
    wb, dwacc, hb, yb, dz, dzr, sb, tb, far1, pure1, merged1, far2, pure2, merged2, ob,
    stat, own, st0, mid, st1, row, st2, lse, lossacc,
    wsem, hsem, rs_send, rs_recv, dz_send, dz_recv, w_send, w_recv,
    st0_send, st0_recv, st1_send, st1_recv, st2_send, st2_recv, osem, dwsem,
):
    vocab, dim = w_hbm.shape
    half = dim // 2
    mt = vocab // 2
    tok = hb.shape[1] * hb.shape[2] * ROWS
    tokc = tok // 2

    me = lax.axis_index(AXIS)
    core = lax.rem(me, 2)
    other = 1 - core
    x = lax.rem(me // 2, side)
    y = me // (2 * side)
    p = x + core * (y - x)
    q = y + core * (x - y)
    partner = me + 1 - 2 * core

    def at_xy(xx, yy):
        return (lax.rem(yy + side, side) * side + lax.rem(xx + side, side)) * 2 + core

    def at_pq(pp, qq):
        return at_xy(pp + core * (qq - pp), qq + core * (pp - qq))

    peers_x = [at_xy(x + k, y) for k in range(1, side)]
    peers_y = [at_xy(x, y + k) for k in range(1, side)]
    to_p, to_q = (at_pq(p + 1, q), at_pq(p - 1, q)), (at_pq(p, q + 1), at_pq(p, q - 1))
    near_p = lax.rem(p + 1, side), lax.rem(p + side - 1, side), lax.rem(p + 2, side)
    near_q = lax.rem(q + 1, side), lax.rem(q + side - 1, side), lax.rem(q + 2, side)

    def rcopy(src, dst, send, recv, dev):
        return pltpu.make_async_remote_copy(
            src_ref=src, dst_ref=dst, send_sem=send, recv_sem=recv,
            device_id={AXIS: dev}, device_id_type=pl.DeviceIdType.MESH,
        )

    def guarded(cond, fn):
        pl.when(cond)(fn)

    barrier = pltpu.get_barrier_semaphore()
    friends = [partner, *peers_x, *peers_y]
    for dev in friends:
        pl.semaphore_signal(barrier, inc=1, device_id={AXIS: dev}, device_id_type=pl.DeviceIdType.MESH)

    def h_copies(c):
        s = lax.rem(c, 4)
        out = []
        for k in range(side):
            out.append(pltpu.make_async_copy(hid.at[:, k, 0, c], hb.at[s, k], hsem.at[s]))
            out.append(pltpu.make_async_copy(hid.at[k, :, 1, c], hb.at[s, side + k], hsem.at[s]))
        return out

    def h_start(c):
        for d in h_copies(c):
            d.start()

    def h_wait(c):
        s = lax.rem(c, 4)
        pltpu.make_async_copy(hb.at[s], hb.at[s], hsem.at[s]).wait()

    w_local = pltpu.make_async_copy(w_hbm, wb.at[core], wsem)
    w_local.start()
    h_start(0)
    dwacc[...] = jnp.zeros_like(dwacc)
    lossacc[...] = jnp.zeros_like(lossacc)
    pl.semaphore_wait(barrier, len(friends))
    w_local.wait()
    w_remote = rcopy(wb.at[core], wb.at[core], w_send, w_recv, partner)
    w_remote.start()

    def rs(kind, c):
        s = lax.rem(c, 2)
        lo, hi = pl.ds(0, half), pl.ds(half, half)
        buf, to, (up, down, far) = (sb, to_p, near_p) if kind < 3 else (tb, to_q, near_q)
        dst = (far1, pure1, merged1, far2, pure2, merged2)[kind]
        src = {0: ((far, lo), (far, hi)), 1: ((up, hi), (down, lo)), 2: ((up, lo), (down, hi))}[kind % 3]
        return [
            rcopy(buf.at[s, src[d][0], :, src[d][1]], dst.at[s, d], rs_send.at[kind, s, d], rs_recv.at[kind, s, d], to[d])
            for d in range(2)
        ]

    def start(ds):
        for d in ds:
            d.start()

    def wait_recv(ds):
        for d in ds:
            d.wait_recv()

    def wait_send(ds):
        for d in ds:
            d.wait_send()

    def dz_copy(c):
        s = lax.rem(c, 2)
        return [rcopy(dz.at[other], dzr.at[s], dz_send, dz_recv.at[s], partner)]

    def st0_copy(i):
        s = lax.rem(i, 2)
        return [rcopy(own.at[s], st0.at[s], st0_send.at[s], st0_recv.at[s], partner)]

    def st1_copy(i):
        s = lax.rem(i, 2)
        return [
            rcopy(mid.at[s], st1.at[s, x], st1_send.at[s, k], st1_recv.at[s, k], peer)
            for k, peer in enumerate(peers_x)
        ]

    def st2_copy(i):
        s = lax.rem(i, 2)
        return [
            rcopy(row.at[s], st2.at[s, y], st2_send.at[s, k], st2_recv.at[s, k], peer)
            for k, peer in enumerate(peers_y)
        ]

    def two(fn):
        lax.fori_loop(0, 2, lambda j, carry: (fn(j), carry)[1], 0)

    def logits(i, j, slot):
        r = pl.ds(pl.multiple_of(j * mt, mt), mt)
        h = hb[lax.rem(i, 4)].reshape(tok, dim)
        yb[slot, r, :] = dot_nt(wb[core, r, :], h) * LOG2E

    def grad_logits(c, j, slot):
        r = pl.ds(pl.multiple_of(j * mt, mt), mt)
        prob = jnp.exp2(yb[slot, r, :] - lse[0:1, :])
        hit = lax.broadcasted_iota(jnp.int32, prob.shape, 0) == tgt[c] - (me * vocab + j * mt)
        g = (prob + jnp.where(hit, -1.0 / tokens, 0.0)).astype(BF16)
        dz[0, r, :] = g[:, :tokc]
        dz[1, r, :] = g[:, tokc:]

    def statistics(i, j, slot):
        v = yb[slot, pl.ds(pl.multiple_of(j * mt, mt), mt), :]
        top = jnp.max(v, axis=0, keepdims=True)
        total = jnp.sum(jnp.exp2(v - top), axis=0, keepdims=True)
        hit = lax.broadcasted_iota(jnp.int32, v.shape, 0) == tgt[lax.rem(i, chunks)] - (me * vocab + j * mt)
        stat[j, 0:1, :] = top + jnp.log(total) * LOG2E
        stat[j, 1:2, :] = jnp.sum(jnp.where(hit, v, 0.0), axis=0, keepdims=True)

    def grad_w(c, k):
        n = dim // 2
        cols = pl.ds(pl.multiple_of(k * n, n), n)
        h = hb[lax.rem(c, 4), :, :, :, cols].reshape(tok, n)
        dwacc[:, cols] += dot_nn(dz[0], h[:tokc]) + dot_nn(dz[1], h[tokc:])

    def grad_h(c):
        s = lax.rem(c, 2)
        v = dot_tn(dz[core], wb[core]) + dot_tn(dzr[s], wb[other])
        sb[s] = v.reshape(side, side * ROWS, dim)

    def finish(c):
        s = lax.rem(c, 2)
        wait_recv(rs(PURE2, c) + rs(MERGED2, c))
        wait_send(rs(FAR2, c) + rs(PURE2, c) + rs(MERGED2, c))
        guarded(c >= 2, lambda: pltpu.make_async_copy(ob.at[s], dh_hbm.at[c - 2], osem.at[s]).wait())
        ob[s, :, :half] = tb[s, q, :, :half] + merged2[s, 0] + pure2[s, 1]
        ob[s, :, half:] = tb[s, q, :, half:] + pure2[s, 0] + merged2[s, 1]
        pltpu.make_async_copy(ob.at[s], dh_hbm.at[c], osem.at[s]).start()

    def turn(c):
        s = lax.rem(c, 2)
        wait_recv(rs(PURE1, c) + rs(MERGED1, c))
        lo = sb[s, p, :, :half] + merged1[s, 0] + pure1[s, 1]
        hi = sb[s, p, :, half:] + pure1[s, 0] + merged1[s, 1]
        tb[s, :, :, :half] = lo.reshape(side, ROWS, half)
        tb[s, :, :, half:] = hi.reshape(side, ROWS, half)
        start(rs(FAR2, c) + rs(PURE2, c))
        wait_send(rs(FAR1, c) + rs(PURE1, c) + rs(MERGED1, c))

    def merge1(c):
        s = lax.rem(c, 2)
        up, down, _ = near_p
        wait_recv(rs(FAR1, c))
        sb[s, up, :, :half] += far1[s, 0]
        sb[s, down, :, half:] += far1[s, 1]
        start(rs(MERGED1, c))

    def merge2(c):
        s = lax.rem(c, 2)
        up, down, _ = near_q
        wait_recv(rs(FAR2, c))
        tb[s, up, :, :half] += far2[s, 0]
        tb[s, down, :, half:] += far2[s, 1]
        start(rs(MERGED2, c))

    def st_own(i):
        s = lax.rem(i, 2)
        guarded(i >= 2, lambda: wait_send(st0_copy(i)))
        own[s, 0:1, :] = join([stat[0, 0:1, :], stat[1, 0:1, :]])
        own[s, 1:2, :] = stat[0, 1:2, :] + stat[1, 1:2, :]
        start(st0_copy(i))

    def st_pair(i):
        s = lax.rem(i, 2)
        wait_recv(st0_copy(i))
        guarded(i >= 2, lambda: wait_send(st1_copy(i)))
        mid[s, 0:1, :] = join([own[s, 0:1, :], st0[s, 0:1, :]])
        mid[s, 1:2, :] = own[s, 1:2, :] + st0[s, 1:2, :]
        st1[s, x] = mid[s]
        start(st1_copy(i))

    def st_row(i):
        s = lax.rem(i, 2)
        wait_recv(st1_copy(i))
        guarded(i >= 2, lambda: wait_send(st2_copy(i)))
        row[s, 0:1, :] = join([st1[s, k, 0:1, :] for k in range(side)])
        row[s, 1:2, :] = functools.reduce(jnp.add, [st1[s, k, 1:2, :] for k in range(side)])
        st2[s, y] = row[s]
        start(st2_copy(i))

    def st_all(i):
        s = lax.rem(i, 2)
        wait_recv(st2_copy(i))
        full = join([st2[s, k, 0:1, :] for k in range(side)])
        hit = functools.reduce(jnp.add, [st2[s, k, 1:2, :] for k in range(side)])
        lse[0:1, :] = full + math.log2(tokens)
        lossacc[...] += full - hit

    def step(i, carry):
        c = i - 2
        slot = lax.rem(i, 2)
        has_a, has_c = i < chunks, jnp.logical_and(c >= 0, c < chunks)

        @pl.when(i + 1 < chunks)
        def _():
            h_start(i + 1)

        @pl.when(has_a)
        def _():
            h_wait(i)

        @pl.when(jnp.logical_and(has_a, has_c))
        def _():
            two(lambda j: (grad_logits(c, j, slot), logits(i, j, slot)))

        @pl.when(jnp.logical_and(has_a, jnp.logical_not(has_c)))
        def _():
            two(lambda j: logits(i, j, slot))
            two(lambda j: statistics(i, j, slot))

        @pl.when(jnp.logical_and(has_c, jnp.logical_not(has_a)))
        def _():
            two(lambda j: grad_logits(c, j, slot))

        def live(k):
            return jnp.logical_and(k >= 0, k < chunks)

        @pl.when(has_c)
        def _():
            start(dz_copy(c))

        guarded(live(c - 3), lambda: finish(c - 3))
        guarded(live(c - 2), lambda: turn(c - 2))
        guarded(live(c - 1), lambda: start(rs(PURE1, c - 1)))
        guarded(live(i - 1), lambda: st_row(i - 1))

        @pl.when(has_c)
        def _():
            two(lambda j: (statistics(i, j, slot), grad_w(c, j)))

        guarded(live(c - 1), lambda: merge1(c - 1))
        guarded(live(c - 2), lambda: merge2(c - 2))
        guarded(has_a, lambda: st_own(i))

        @pl.when(has_c)
        def _():
            guarded(c == 0, w_remote.wait_recv)
            wait_recv(dz_copy(c))
            grad_h(c)

        guarded(has_a, lambda: st_pair(i))

        @pl.when(has_c)
        def _():
            start(rs(FAR1, c))
            wait_send(dz_copy(c))

        guarded(live(i - 1), lambda: st_all(i - 1))

        @pl.when(c == chunks - 1)
        def _():
            pltpu.make_async_copy(dwacc, dw_hbm, dwsem).start()

        return carry

    lax.fori_loop(0, chunks + 5, step, 0)

    for i in range(max(chunks - 2, 0), chunks):
        wait_send(st0_copy(i) + st1_copy(i) + st2_copy(i))
        pltpu.make_async_copy(ob.at[i % 2], dh_hbm.at[i], osem.at[i % 2]).wait()
    w_remote.wait_send()
    pltpu.make_async_copy(dwacc, dw_hbm, dwsem).wait()
    loss_ref[...] = jnp.broadcast_to(jnp.sum(lossacc[...], axis=1, keepdims=True) * (LN2 / tokens), loss_ref.shape)


def solution(mesh):
    group = mesh.shape[AXIS]
    side = math.isqrt(group // 2)

    def local_step(hidden, targets, w_blk):
        tokens, dim = hidden.shape
        vocab = w_blk.shape[0]
        chunks = tokens // group // ROWS
        tok = group * ROWS
        half = dim // 2
        hid = hidden.reshape(side, side, 2, chunks, ROWS, dim)
        t = targets.reshape(side, side, 2, chunks, ROWS)
        tgt = jnp.concatenate(
            [t[:, :, 0].transpose(2, 1, 0, 3).reshape(chunks, 1, tok // 2), t[:, :, 1].transpose(2, 0, 1, 3).reshape(chunks, 1, tok // 2)],
            axis=2,
        )
        dma = pltpu.SemaphoreType.DMA
        any_spec = pl.BlockSpec(memory_space=pl.ANY)
        vmem_spec = pl.BlockSpec(memory_space=pltpu.VMEM)
        big, small = (2, 2, side * ROWS, half), (2, 2, ROWS, half)
        loss, dh, dw = pl.pallas_call(
            functools.partial(head_kernel, group, side, chunks, tokens),
            out_shape=(
                jax.ShapeDtypeStruct((1, 128), F32),
                jax.ShapeDtypeStruct((chunks, ROWS, dim), F32),
                jax.ShapeDtypeStruct((vocab, dim), F32),
            ),
            in_specs=[any_spec, vmem_spec, any_spec],
            out_specs=(vmem_spec, any_spec, any_spec),
            scratch_shapes=[
                pltpu.VMEM((2, vocab, dim), BF16),
                pltpu.VMEM((vocab, dim), F32),
                pltpu.VMEM((4, 2 * side, side, ROWS, dim), BF16),
                pltpu.VMEM((2, vocab, tok), F32),
                pltpu.VMEM((2, vocab, tok // 2), BF16),
                pltpu.VMEM((2, vocab, tok // 2), BF16),
                pltpu.VMEM((2, side, side * ROWS, dim), F32),
                pltpu.VMEM((2, side, ROWS, dim), F32),
                *[pltpu.VMEM(big, F32)] * 3,
                *[pltpu.VMEM(small, F32)] * 3,
                pltpu.VMEM((2, ROWS, dim), F32),
                pltpu.VMEM((2, 2, tok), F32),
                pltpu.VMEM((2, 2, tok), F32),
                pltpu.VMEM((2, 2, tok), F32),
                pltpu.VMEM((2, 2, tok), F32),
                pltpu.VMEM((2, side, 2, tok), F32),
                pltpu.VMEM((2, 2, tok), F32),
                pltpu.VMEM((2, side, 2, tok), F32),
                pltpu.VMEM((1, tok), F32),
                pltpu.VMEM((1, tok), F32),
                dma, dma((4,)),
                dma((6, 2, 2)), dma((6, 2, 2)),
                dma, dma((2,)), dma, dma,
                dma((2,)), dma((2,)),
                dma((2, side - 1)), dma((2, side - 1)),
                dma((2, side - 1)), dma((2, side - 1)),
                dma((2,)), dma,
            ],
            compiler_params=pltpu.CompilerParams(
                collective_id=0, has_side_effects=True, vmem_limit_bytes=67043328,
            ),
            name="head",
        )(hid, tgt, w_blk)
        return loss[0, :1], dh.reshape(tokens // group, dim), dw

    return jax.shard_map(
        local_step,
        mesh=mesh,
        in_specs=(P("data", None), P("data"), P(AXIS, None)),
        out_specs=(P("data"), P(("data", AXIS), None), P(("data", AXIS), None)),
        check_vma=False,
    )
```

```python
import functools
import math

import jax
import jax.numpy as jnp
from jax import lax
from jax.experimental import pallas as pl
from jax.experimental.pallas import tpu as pltpu
from jax.sharding import PartitionSpec as P

F32 = jnp.float32
BF16 = jnp.bfloat16
LOG2E = 1.4426950408889634
LN2 = 0.6931471805599453
LATER = 3
ROWS = 16
AXIS = "fsdp"

FAR1, PURE1, MERGED1, FAR2, PURE2, MERGED2 = range(6)


def dot_nt(a, b):
    return lax.dot_general(a, b, (((1,), (1,)), ((), ())), preferred_element_type=F32)


def dot_nn(a, b):
    return lax.dot_general(a, b, (((1,), (0,)), ((), ())), preferred_element_type=F32)


def dot_tn(a, b):
    return lax.dot_general(a, b, (((0,), (0,)), ((), ())), preferred_element_type=F32)


def join(parts):
    top = functools.reduce(jnp.maximum, parts)
    total = functools.reduce(jnp.add, [jnp.exp2(v - top) for v in parts])
    return top + jnp.log(total) * LOG2E


def head_kernel(
    group, side, chunks, tokens,
    hid, tgt, w_hbm,
    loss_ref, dh_hbm, dw_hbm, dz_hbm,
    wb, dwacc, hb, yb, dz, dzr, sb, tb, far1, pure1, merged1, far2, pure2, merged2, ob,
    stat, own, st0, mid, st1, row, st2, lse, lossacc,
    wsem, hsem, rs_send, rs_recv, dz_send, dz_recv, w_send, w_recv,
    st0_send, st0_recv, st1_send, st1_recv, st2_send, st2_recv, osem, dwsem, dxsem,
):
    vocab, dim = w_hbm.shape
    half = dim // 2
    mt = vocab // 2
    stride = chunks // (LATER + 1)
    tok = hb.shape[1] * hb.shape[2] * ROWS
    tokc = tok // 2

    me = lax.axis_index(AXIS)
    core = lax.rem(me, 2)
    other = 1 - core
    x = lax.rem(me // 2, side)
    y = me // (2 * side)
    p = x + core * (y - x)
    q = y + core * (x - y)
    partner = me + 1 - 2 * core
    one = 1 + me // group

    def at_xy(xx, yy):
        return (lax.rem(yy + side, side) * side + lax.rem(xx + side, side)) * 2 + core

    def at_pq(pp, qq):
        return at_xy(pp + core * (qq - pp), qq + core * (pp - qq))

    peers_x = [at_xy(x + k, y) for k in range(1, side)]
    peers_y = [at_xy(x, y + k) for k in range(1, side)]
    to_p, to_q = (at_pq(p + 1, q), at_pq(p - 1, q)), (at_pq(p, q + 1), at_pq(p, q - 1))
    near_p = lax.rem(p + 1, side), lax.rem(p + side - 1, side), lax.rem(p + 2, side)
    near_q = lax.rem(q + 1, side), lax.rem(q + side - 1, side), lax.rem(q + 2, side)

    def rcopy(src, dst, send, recv, dev):
        return pltpu.make_async_remote_copy(
            src_ref=src, dst_ref=dst, send_sem=send, recv_sem=recv,
            device_id={AXIS: dev}, device_id_type=pl.DeviceIdType.MESH,
        )

    def guarded(cond, fn):
        pl.when(cond)(fn)

    barrier = pltpu.get_barrier_semaphore()
    friends = [partner, *peers_x, *peers_y]
    for dev in friends:
        pl.semaphore_signal(barrier, inc=1, device_id={AXIS: dev}, device_id_type=pl.DeviceIdType.MESH)

    def h_copies(c):
        s = lax.rem(c, 4)
        out = []
        for k in range(side):
            out.append(pltpu.make_async_copy(hid.at[:, k, 0, c], hb.at[s, k], hsem.at[s]))
            out.append(pltpu.make_async_copy(hid.at[k, :, 1, c], hb.at[s, side + k], hsem.at[s]))
        return out

    def h_start(c):
        for d in h_copies(c):
            d.start()

    def h_wait(c):
        s = lax.rem(c, 4)
        pltpu.make_async_copy(hb.at[s], hb.at[s], hsem.at[s]).wait()

    w_local = pltpu.make_async_copy(w_hbm, wb.at[core], wsem)
    w_local.start()
    h_start(0)
    dwacc[...] = jnp.zeros_like(dwacc)
    lossacc[...] = jnp.zeros_like(lossacc)
    pl.semaphore_wait(barrier, len(friends))
    w_local.wait()
    w_remote = rcopy(wb.at[core], wb.at[core], w_send, w_recv, partner)
    w_remote.start()

    def rs(kind, c):
        s = lax.rem(c, 2)
        lo, hi = pl.ds(0, half), pl.ds(half, half)
        buf, to, (up, down, far) = (sb, to_p, near_p) if kind < 3 else (tb, to_q, near_q)
        dst = (far1, pure1, merged1, far2, pure2, merged2)[kind]
        src = {0: ((far, lo), (far, hi)), 1: ((up, hi), (down, lo)), 2: ((up, lo), (down, hi))}[kind % 3]
        return [
            rcopy(buf.at[s, src[d][0], :, src[d][1]], dst.at[s, d], rs_send.at[kind, s, d], rs_recv.at[kind, s, d], to[d])
            for d in range(2)
        ]

    def start(ds):
        for d in ds:
            d.start()

    def wait_recv(ds):
        for d in ds:
            d.wait_recv()

    def wait_send(ds):
        for d in ds:
            d.wait_send()

    def dz_copy(c):
        s = lax.rem(c, 2)
        return [rcopy(dz.at[s, other], dzr.at[s], dz_send, dz_recv.at[s], partner)]

    def st0_copy(i):
        s = lax.rem(i, 2)
        return [rcopy(own.at[s], st0.at[s], st0_send.at[s], st0_recv.at[s], partner)]

    def st1_copy(i):
        s = lax.rem(i, 2)
        return [
            rcopy(mid.at[s], st1.at[s, x], st1_send.at[s, k], st1_recv.at[s, k], peer)
            for k, peer in enumerate(peers_x)
        ]

    def st2_copy(i):
        s = lax.rem(i, 2)
        return [
            rcopy(row.at[s], st2.at[s, y], st2_send.at[s, k], st2_recv.at[s, k], peer)
            for k, peer in enumerate(peers_y)
        ]

    def two(fn):
        lax.fori_loop(0, 2, lambda j, carry: (fn(j), carry)[1], 0)

    def logits(i, j, slot):
        r = pl.ds(pl.multiple_of(j * mt, mt), mt)
        h = hb[lax.rem(i, 4)].reshape(tok, dim)
        yb[slot, r, :] = dot_nt(wb[core, r, :], h) * LOG2E

    def grad_logits(c, j, slot):
        r = pl.ds(pl.multiple_of(j * mt, mt), mt)
        prob = jnp.exp2(yb[slot, r, :] - lse[0:1, :])
        hit = lax.broadcasted_iota(jnp.int32, prob.shape, 0) == tgt[c] - (me * vocab + j * mt)
        g = (prob + jnp.where(hit, -1.0 / tokens, 0.0)).astype(BF16)
        dz[slot, 0, r, :] = g[:, :tokc]
        dz[slot, 1, r, :] = g[:, tokc:]

    def statistics(i, j, slot):
        v = yb[slot, pl.ds(pl.multiple_of(j * mt, mt), mt), :]
        top = jnp.max(v, axis=0, keepdims=True)
        total = jnp.sum(jnp.exp2(v - top), axis=0, keepdims=True)
        hit = lax.broadcasted_iota(jnp.int32, v.shape, 0) == tgt[lax.rem(i, chunks)] - (me * vocab + j * mt)
        stat[j, 0:1, :] = top + jnp.log(total) * LOG2E
        stat[j, 1:2, :] = jnp.sum(jnp.where(hit, v, 0.0), axis=0, keepdims=True)

    def grad_w(c, k):
        n = dim // 2
        cols = pl.ds(pl.multiple_of(k * n, n), n)
        h = hb[lax.rem(c, 4), :, :, :, cols].reshape(tok, n)
        s = lax.rem(c, 2)
        dwacc[:, cols] += dot_nn(dz[s, 0], h[:tokc]) + dot_nn(dz[s, 1], h[tokc:])

    def grad_h(c):
        s = lax.rem(c, 2)
        v = dot_tn(dz[s, core], wb[core]) + dot_tn(dzr[s], wb[other])
        sb[s] = v.reshape(side, side * ROWS, dim)

    def finish(c):
        s = lax.rem(c, 2)
        wait_recv(rs(PURE2, c) + rs(MERGED2, c))
        wait_send(rs(FAR2, c) + rs(PURE2, c) + rs(MERGED2, c))
        guarded(c >= 2, lambda: pltpu.make_async_copy(ob.at[s], dh_hbm.at[c - 2], osem.at[s]).wait())
        ob[s, :, :half] = tb[s, q, :, :half] + merged2[s, 0] + pure2[s, 1]
        ob[s, :, half:] = tb[s, q, :, half:] + pure2[s, 0] + merged2[s, 1]
        pltpu.make_async_copy(ob.at[s], dh_hbm.at[c], osem.at[s]).start()

    def turn(c):
        s = lax.rem(c, 2)
        wait_recv(rs(PURE1, c) + rs(MERGED1, c))
        lo = sb[s, p, :, :half] + merged1[s, 0] + pure1[s, 1]
        hi = sb[s, p, :, half:] + pure1[s, 0] + merged1[s, 1]
        tb[s, :, :, :half] = lo.reshape(side, ROWS, half)
        tb[s, :, :, half:] = hi.reshape(side, ROWS, half)
        start(rs(FAR2, c) + rs(PURE2, c))
        wait_send(rs(FAR1, c) + rs(PURE1, c) + rs(MERGED1, c))

    def merge1(c):
        s = lax.rem(c, 2)
        up, down, _ = near_p
        wait_recv(rs(FAR1, c))
        sb[s, up, :, :half] += far1[s, 0]
        sb[s, down, :, half:] += far1[s, 1]
        start(rs(MERGED1, c))

    def merge2(c):
        s = lax.rem(c, 2)
        up, down, _ = near_q
        wait_recv(rs(FAR2, c))
        tb[s, up, :, :half] += far2[s, 0]
        tb[s, down, :, half:] += far2[s, 1]
        start(rs(MERGED2, c))

    def st_own(i):
        s = lax.rem(i, 2)
        guarded(i >= 2, lambda: wait_send(st0_copy(i)))
        own[s, 0:1, :] = join([stat[0, 0:1, :], stat[1, 0:1, :]])
        own[s, 1:2, :] = stat[0, 1:2, :] + stat[1, 1:2, :]
        start(st0_copy(i))

    def st_pair(i):
        s = lax.rem(i, 2)
        wait_recv(st0_copy(i))
        guarded(i >= 2, lambda: wait_send(st1_copy(i)))
        mid[s, 0:1, :] = join([own[s, 0:1, :], st0[s, 0:1, :]])
        mid[s, 1:2, :] = own[s, 1:2, :] + st0[s, 1:2, :]
        st1[s, x] = mid[s]
        start(st1_copy(i))

    def st_row(i):
        s = lax.rem(i, 2)
        wait_recv(st1_copy(i))
        guarded(i >= 2, lambda: wait_send(st2_copy(i)))
        row[s, 0:1, :] = join([st1[s, k, 0:1, :] for k in range(side)])
        row[s, 1:2, :] = functools.reduce(jnp.add, [st1[s, k, 1:2, :] for k in range(side)])
        st2[s, y] = row[s]
        start(st2_copy(i))

    def st_all(i):
        s = lax.rem(i, 2)
        wait_recv(st2_copy(i))
        full = join([st2[s, k, 0:1, :] for k in range(side)])
        hit = functools.reduce(jnp.add, [st2[s, k, 1:2, :] for k in range(side)])
        lse[0:1, :] = full + math.log2(tokens)
        lossacc[...] += full - hit

    def step(i, carry):
        c = i - 2
        slot = lax.rem(i, 2)
        has_a, has_c = i < chunks, jnp.logical_and(c >= 0, c < chunks)

        @pl.when(i + 1 < chunks)
        def _():
            h_start(i + 1)

        @pl.when(has_a)
        def _():
            h_wait(i)

        @pl.when(jnp.logical_and(has_a, has_c))
        def _():
            two(lambda j: (grad_logits(c, j, slot), logits(i, j, slot)))

        @pl.when(jnp.logical_and(has_a, jnp.logical_not(has_c)))
        def _():
            two(lambda j: logits(i, j, slot))
            two(lambda j: statistics(i, j, slot))

        @pl.when(jnp.logical_and(has_c, jnp.logical_not(has_a)))
        def _():
            two(lambda j: grad_logits(c, j, slot))

        def live(k):
            return jnp.logical_and(k >= 0, k < chunks)

        @pl.when(has_c)
        def _():
            start(dz_copy(c))

        guarded(live(c - 3), lambda: finish(c - 3))
        guarded(live(c - 2), lambda: turn(c - 2))
        guarded(live(c - 1), lambda: start(rs(PURE1, c - 1)))
        later = jnp.logical_and(lax.rem(c, stride) == stride - 1, c // stride < LATER)
        now = jnp.logical_and(jnp.logical_and(c >= 0, c < chunks - 2), jnp.logical_not(later))
        save = jnp.logical_and(jnp.logical_and(c >= 0, c < chunks - 2), later)

        @pl.when(now)
        def _():
            def half_dw(j):
                statistics(i, j, slot)
                grad_w(c, j)

            lax.fori_loop(0, one, lambda j, u: (half_dw(j), u)[1], 0)
            guarded(live(i - 1), lambda: st_row(i - 1))
            lax.fori_loop(one, 2, lambda j, u: (half_dw(j), u)[1], 0)

        @pl.when(jnp.logical_not(now))
        def _():
            @pl.when(save)
            def _():
                pltpu.make_async_copy(dz.at[lax.rem(c + 2, 2)], dz_hbm.at[c // stride], dxsem).start()
                two(lambda j: statistics(i, j, slot))

            guarded(live(i - 1), lambda: st_row(i - 1))

        @pl.when(c == chunks)
        def _():
            two(lambda j: grad_w(c - 2, j))

        guarded(live(c - 1), lambda: merge1(c - 1))
        guarded(live(c - 2), lambda: merge2(c - 2))
        guarded(has_a, lambda: st_own(i))

        @pl.when(has_c)
        def _():
            guarded(c == 0, w_remote.wait_recv)
            wait_recv(dz_copy(c))
            grad_h(c)

        guarded(has_a, lambda: st_pair(i))

        @pl.when(has_c)
        def _():
            start(rs(FAR1, c))
            wait_send(dz_copy(c))

        @pl.when(save)
        def _():
            pltpu.make_async_copy(dz.at[lax.rem(c + 2, 2)], dz_hbm.at[c // stride], dxsem).wait()

        guarded(live(i - 1), lambda: st_all(i - 1))

        @pl.when(c == chunks)
        def _():
            two(lambda j: grad_w(c - 1, j))
            pltpu.make_async_copy(dwacc, dw_hbm, dwsem).start()

        return carry

    lax.fori_loop(0, chunks + 5, step, 0)

    for i in range(max(chunks - 2, 0), chunks):
        wait_send(st0_copy(i) + st1_copy(i) + st2_copy(i))
        pltpu.make_async_copy(ob.at[i % 2], dh_hbm.at[i], osem.at[i % 2]).wait()
    w_remote.wait_send()
    pltpu.make_async_copy(dwacc, dw_hbm, dwsem).wait()
    loss_ref[...] = jnp.broadcast_to(jnp.sum(lossacc[...], axis=1, keepdims=True) * (LN2 / tokens), loss_ref.shape)


def last_kernel(side, dw_ref, dh_ref, dz_ref, *rest):
    hid, (dw_out, dh_out) = rest[:LATER], rest[LATER:]
    total = dw_ref[...]
    for k in range(LATER):
        h = hid[k]
        by_x = [h[yy, xx, 0, 0] for xx in range(side) for yy in range(side)]
        by_y = [h[yy, xx, 1, 0] for yy in range(side) for xx in range(side)]
        total += dot_nn(dz_ref[k, 0], jnp.concatenate(by_x, axis=0)) + dot_nn(dz_ref[k, 1], jnp.concatenate(by_y, axis=0))
    dw_out[...] = total
    dh_out[...] = dh_ref[...]


def solution(mesh):
    group = mesh.shape[AXIS]
    side = math.isqrt(group // 2)

    def local_step(hidden, targets, w_blk):
        tokens, dim = hidden.shape
        vocab = w_blk.shape[0]
        chunks = tokens // group // ROWS
        tok = group * ROWS
        half = dim // 2
        hid = hidden.reshape(side, side, 2, chunks, ROWS, dim)
        t = targets.reshape(side, side, 2, chunks, ROWS)
        tgt = jnp.concatenate(
            [t[:, :, 0].transpose(2, 1, 0, 3).reshape(chunks, 1, tok // 2), t[:, :, 1].transpose(2, 0, 1, 3).reshape(chunks, 1, tok // 2)],
            axis=2,
        )
        dma = pltpu.SemaphoreType.DMA
        any_spec = pl.BlockSpec(memory_space=pl.ANY)
        vmem_spec = pl.BlockSpec(memory_space=pltpu.VMEM)
        big, small = (2, 2, side * ROWS, half), (2, 2, ROWS, half)
        loss, dh, dw, dz_left = pl.pallas_call(
            functools.partial(head_kernel, group, side, chunks, tokens),
            out_shape=(
                jax.ShapeDtypeStruct((1, 128), F32),
                jax.ShapeDtypeStruct((chunks, ROWS, dim), F32),
                jax.ShapeDtypeStruct((vocab, dim), F32),
                jax.ShapeDtypeStruct((LATER, 2, vocab, tok // 2), BF16),
            ),
            in_specs=[any_spec, vmem_spec, any_spec],
            out_specs=(vmem_spec, any_spec, any_spec, any_spec),
            scratch_shapes=[
                pltpu.VMEM((2, vocab, dim), BF16),
                pltpu.VMEM((vocab, dim), F32),
                pltpu.VMEM((4, 2 * side, side, ROWS, dim), BF16),
                pltpu.VMEM((2, vocab, tok), F32),
                pltpu.VMEM((2, 2, vocab, tok // 2), BF16),
                pltpu.VMEM((2, vocab, tok // 2), BF16),
                pltpu.VMEM((2, side, side * ROWS, dim), F32),
                pltpu.VMEM((2, side, ROWS, dim), F32),
                *[pltpu.VMEM(big, F32)] * 3,
                *[pltpu.VMEM(small, F32)] * 3,
                pltpu.VMEM((2, ROWS, dim), F32),
                pltpu.VMEM((2, 2, tok), F32),
                pltpu.VMEM((2, 2, tok), F32),
                pltpu.VMEM((2, 2, tok), F32),
                pltpu.VMEM((2, 2, tok), F32),
                pltpu.VMEM((2, side, 2, tok), F32),
                pltpu.VMEM((2, 2, tok), F32),
                pltpu.VMEM((2, side, 2, tok), F32),
                pltpu.VMEM((1, tok), F32),
                pltpu.VMEM((1, tok), F32),
                dma, dma((4,)),
                dma((6, 2, 2)), dma((6, 2, 2)),
                dma, dma((2,)), dma, dma,
                dma((2,)), dma((2,)),
                dma((2, side - 1)), dma((2, side - 1)),
                dma((2, side - 1)), dma((2, side - 1)),
                dma((2,)), dma, dma,
            ],
            compiler_params=pltpu.CompilerParams(
                collective_id=0, has_side_effects=True, vmem_limit_bytes=67043328,
            ),
            name="head",
        )(hid, tgt, w_blk)
        steps, cols = 8, dim // 8
        rows = tokens // group // steps
        stride = chunks // (LATER + 1)
        dw_spec, dh_spec = pl.BlockSpec((vocab, cols), lambda j: (0, j)), pl.BlockSpec((rows, dim), lambda j: (j, 0))
        h_specs = [
            pl.BlockSpec((side, side, 2, 1, ROWS, cols), lambda j, k=k: (0, 0, 0, (k + 1) * stride - 1, 0, j)) for k in range(LATER)
        ]
        dw, dh = pl.pallas_call(
            functools.partial(last_kernel, side),
            grid=(steps,),
            out_shape=(jax.ShapeDtypeStruct((vocab, dim), F32), jax.ShapeDtypeStruct((tokens // group, dim), F32)),
            in_specs=[dw_spec, dh_spec, pl.BlockSpec((LATER, 2, vocab, tok // 2), lambda j: (0, 0, 0, 0)), *h_specs],
            out_specs=(dw_spec, dh_spec),
            compiler_params=pltpu.CompilerParams(dimension_semantics=("arbitrary",), vmem_limit_bytes=48 << 20),
            name="last",
        )(dw, dh.reshape(tokens // group, dim), dz_left, *[hid] * LATER)
        return loss[0, :1], dh, dw

    return jax.shard_map(
        local_step,
        mesh=mesh,
        in_specs=(P("data", None), P("data"), P(AXIS, None)),
        out_specs=(P("data"), P(("data", AXIS), None), P(("data", AXIS), None)),
        check_vma=False,
    )
```

```python
import functools
import math

import jax
import jax.numpy as jnp
from jax import lax
from jax.experimental import pallas as pl
from jax.experimental.pallas import tpu as pltpu
from jax.sharding import PartitionSpec as P

F32 = jnp.float32
BF16 = jnp.bfloat16
LOG2E = 1.4426950408889634
LN2 = 0.6931471805599453
LATER = 2
ROWS = 16
AXIS = "fsdp"

FAR1, PURE1, MERGED1, FAR2, PURE2, MERGED2 = range(6)


def dot_nt(a, b):
    return lax.dot_general(a, b, (((1,), (1,)), ((), ())), preferred_element_type=F32)


def dot_nn(a, b):
    return lax.dot_general(a, b, (((1,), (0,)), ((), ())), preferred_element_type=F32)


def dot_tn(a, b):
    return lax.dot_general(a, b, (((0,), (0,)), ((), ())), preferred_element_type=F32)


def join(parts):
    top = functools.reduce(jnp.maximum, parts)
    total = functools.reduce(jnp.add, [jnp.exp2(v - top) for v in parts])
    return top + jnp.log(total) * LOG2E


def head_kernel(
    group, side, chunks, tokens,
    hid, tgt, w_hbm,
    loss_ref, dh_hbm, dw_hbm, dz_hbm,
    wb, dwacc, hb, yb, dz, dzr, sb, tb, far1, pure1, merged1, far2, pure2, merged2, ob,
    stat, own, st0, mid, st1, row, st2, lse, lossacc,
    wsem, hsem, rs_send, rs_recv, dz_send, dz_recv, w_send, w_recv,
    st0_send, st0_recv, st1_send, st1_recv, st2_send, st2_recv, osem, dwsem, dxsem,
):
    vocab, dim = w_hbm.shape
    half = dim // 2
    mt = vocab // 2
    stride = chunks // (LATER + 1)
    tok = hb.shape[1] * hb.shape[2] * ROWS
    tokc = tok // 2

    me = lax.axis_index(AXIS)
    core = lax.rem(me, 2)
    other = 1 - core
    x = lax.rem(me // 2, side)
    y = me // (2 * side)
    p = x + core * (y - x)
    q = y + core * (x - y)
    partner = me + 1 - 2 * core
    one = 1 + me // group

    def at_xy(xx, yy):
        return (lax.rem(yy + side, side) * side + lax.rem(xx + side, side)) * 2 + core

    def at_pq(pp, qq):
        return at_xy(pp + core * (qq - pp), qq + core * (pp - qq))

    peers_x = [at_xy(x + k, y) for k in range(1, side)]
    peers_y = [at_xy(x, y + k) for k in range(1, side)]
    to_p, to_q = (at_pq(p + 1, q), at_pq(p - 1, q)), (at_pq(p, q + 1), at_pq(p, q - 1))
    near_p = lax.rem(p + 1, side), lax.rem(p + side - 1, side), lax.rem(p + 2, side)
    near_q = lax.rem(q + 1, side), lax.rem(q + side - 1, side), lax.rem(q + 2, side)

    def rcopy(src, dst, send, recv, dev):
        return pltpu.make_async_remote_copy(
            src_ref=src, dst_ref=dst, send_sem=send, recv_sem=recv,
            device_id={AXIS: dev}, device_id_type=pl.DeviceIdType.MESH,
        )

    def guarded(cond, fn):
        pl.when(cond)(fn)

    barrier = pltpu.get_barrier_semaphore()
    friends = [partner] + [peer + o for peer in (*peers_x, *peers_y) for o in (0, 1 - 2 * core)]
    for dev in friends:
        pl.semaphore_signal(barrier, inc=1, device_id={AXIS: dev}, device_id_type=pl.DeviceIdType.MESH)

    def h_copies(c):
        s = lax.rem(c, 4)
        out = []
        for k in range(side):
            out.append(pltpu.make_async_copy(hid.at[:, k, 0, c], hb.at[s, k], hsem.at[s]))
            out.append(pltpu.make_async_copy(hid.at[k, :, 1, c], hb.at[s, side + k], hsem.at[s]))
        return out

    def h_start(c):
        for d in h_copies(c):
            d.start()

    def h_wait(c):
        s = lax.rem(c, 4)
        pltpu.make_async_copy(hb.at[s], hb.at[s], hsem.at[s]).wait()

    w_local = pltpu.make_async_copy(w_hbm, wb.at[core], wsem)
    w_local.start()
    h_start(0)
    dwacc[...] = jnp.zeros_like(dwacc)
    lossacc[...] = jnp.zeros_like(lossacc)
    pl.semaphore_wait(barrier, len(friends))
    w_local.wait()
    w_remote = rcopy(wb.at[core], wb.at[core], w_send, w_recv, partner)
    w_remote.start()

    def rs(kind, c):
        s = lax.rem(c, 2)
        lo, hi = pl.ds(0, half), pl.ds(half, half)
        buf, to, (up, down, far) = (sb, to_p, near_p) if kind < 3 else (tb, to_q, near_q)
        dst = (far1, pure1, merged1, far2, pure2, merged2)[kind]
        src = {0: ((far, lo), (far, hi)), 1: ((up, hi), (down, lo)), 2: ((up, lo), (down, hi))}[kind % 3]
        return [
            rcopy(buf.at[s, src[d][0], :, src[d][1]], dst.at[s, d], rs_send.at[kind, s, d], rs_recv.at[kind, s, d], to[d])
            for d in range(2)
        ]

    def start(ds):
        for d in ds:
            d.start()

    def wait_recv(ds):
        for d in ds:
            d.wait_recv()

    def wait_send(ds):
        for d in ds:
            d.wait_send()

    def dz_copy(c):
        s = lax.rem(c, 2)
        return [rcopy(dz.at[s, other], dzr.at[s], dz_send, dz_recv.at[s], partner)]

    def st0_copy(i):
        s = lax.rem(i, 2)
        return [rcopy(own.at[s], st0.at[s], st0_send.at[s], st0_recv.at[s], partner)]

    def st1_copy(i):
        s = lax.rem(i, 2)
        to = [(peer - o, k) for k, peer in enumerate(peers_x) for o in (0, 1)] + [(partner, side - 1)]
        return [rcopy(mid.at[s], st1.at[s, x], st1_send.at[s, n], st1_recv.at[s, k], dev) for n, (dev, k) in enumerate(to)]

    def st2_copy(i):
        s = lax.rem(i, 2)
        to = [(peer + o, k) for k, peer in enumerate(peers_y) for o in (0, 1)] + [(partner, side - 1)]
        return [rcopy(row.at[s], st2.at[s, y], st2_send.at[s, n], st2_recv.at[s, k], dev) for n, (dev, k) in enumerate(to)]

    def st_wait(copies, partner_core):
        wait_recv(copies[0:-1:2])
        guarded(core == partner_core, lambda: wait_recv(copies[-1:]))

    def two(fn):
        lax.fori_loop(0, 2, lambda j, carry: (fn(j), carry)[1], 0)

    def logits(i, j, slot):
        r = pl.ds(pl.multiple_of(j * mt, mt), mt)
        h = hb[lax.rem(i, 4)].reshape(tok, dim)
        yb[slot, r, :] = dot_nt(wb[core, r, :], h) * LOG2E

    def grad_logits(c, j, slot):
        r = pl.ds(pl.multiple_of(j * mt, mt), mt)
        prob = jnp.exp2(yb[slot, r, :] - lse[0:1, :])
        hit = lax.broadcasted_iota(jnp.int32, prob.shape, 0) == tgt[c] - (me * vocab + j * mt)
        g = (prob + jnp.where(hit, -1.0 / tokens, 0.0)).astype(BF16)
        dz[slot, 0, r, :] = g[:, :tokc]
        dz[slot, 1, r, :] = g[:, tokc:]

    def statistics(i, j, slot):
        v = yb[slot, pl.ds(pl.multiple_of(j * mt, mt), mt), :]
        top = jnp.max(v, axis=0, keepdims=True)
        total = jnp.sum(jnp.exp2(v - top), axis=0, keepdims=True)
        hit = lax.broadcasted_iota(jnp.int32, v.shape, 0) == tgt[lax.rem(i, chunks)] - (me * vocab + j * mt)
        stat[j, 0:1, :] = top + jnp.log(total) * LOG2E
        stat[j, 1:2, :] = jnp.sum(jnp.where(hit, v, 0.0), axis=0, keepdims=True)

    def grad_w(c, k):
        n = dim // 2
        cols = pl.ds(pl.multiple_of(k * n, n), n)
        h = hb[lax.rem(c, 4), :, :, :, cols].reshape(tok, n)
        s = lax.rem(c, 2)
        dwacc[:, cols] += dot_nn(dz[s, 0], h[:tokc]) + dot_nn(dz[s, 1], h[tokc:])

    def grad_h(c):
        s = lax.rem(c, 2)
        v = dot_tn(dz[s, core], wb[core]) + dot_tn(dzr[s], wb[other])
        sb[s] = v.reshape(side, side * ROWS, dim)

    def finish(c):
        s = lax.rem(c, 2)
        wait_recv(rs(PURE2, c) + rs(MERGED2, c))
        wait_send(rs(FAR2, c) + rs(PURE2, c) + rs(MERGED2, c))
        guarded(c >= 2, lambda: pltpu.make_async_copy(ob.at[s], dh_hbm.at[c - 2], osem.at[s]).wait())
        ob[s, :, :half] = tb[s, q, :, :half] + merged2[s, 0] + pure2[s, 1]
        ob[s, :, half:] = tb[s, q, :, half:] + pure2[s, 0] + merged2[s, 1]
        pltpu.make_async_copy(ob.at[s], dh_hbm.at[c], osem.at[s]).start()

    def turn(c):
        s = lax.rem(c, 2)
        wait_recv(rs(PURE1, c) + rs(MERGED1, c))
        lo = sb[s, p, :, :half] + merged1[s, 0] + pure1[s, 1]
        hi = sb[s, p, :, half:] + pure1[s, 0] + merged1[s, 1]
        tb[s, :, :, :half] = lo.reshape(side, ROWS, half)
        tb[s, :, :, half:] = hi.reshape(side, ROWS, half)
        start(rs(FAR2, c) + rs(PURE2, c))
        wait_send(rs(FAR1, c) + rs(PURE1, c) + rs(MERGED1, c))

    def merge1(c):
        s = lax.rem(c, 2)
        up, down, _ = near_p
        wait_recv(rs(FAR1, c))
        sb[s, up, :, :half] += far1[s, 0]
        sb[s, down, :, half:] += far1[s, 1]
        start(rs(MERGED1, c))

    def merge2(c):
        s = lax.rem(c, 2)
        up, down, _ = near_q
        wait_recv(rs(FAR2, c))
        tb[s, up, :, :half] += far2[s, 0]
        tb[s, down, :, half:] += far2[s, 1]
        start(rs(MERGED2, c))

    def st_own(i):
        s = lax.rem(i, 2)

        @pl.when(core == 0)
        def _():
            guarded(i >= 2, lambda: wait_send(st0_copy(i)))

        own[s, 0:1, :] = join([stat[0, 0:1, :], stat[1, 0:1, :]])
        own[s, 1:2, :] = stat[0, 1:2, :] + stat[1, 1:2, :]
        guarded(core == 0, lambda: start(st0_copy(i)))

    def st_pair(i):
        s = lax.rem(i, 2)

        @pl.when(core == 1)
        def _():
            wait_recv(st0_copy(i))
            guarded(i >= 2, lambda: wait_send(st1_copy(i)))
            mid[s, 0:1, :] = join([st0[s, 0:1, :], own[s, 0:1, :]])
            mid[s, 1:2, :] = st0[s, 1:2, :] + own[s, 1:2, :]
            start(st1_copy(i))

    def st_row(i):
        s = lax.rem(i, 2)
        st_wait(st1_copy(i), 0)

        @pl.when(core == 0)
        def _():
            guarded(i >= 2, lambda: wait_send(st2_copy(i)))
            row[s, 0:1, :] = join([st1[s, k, 0:1, :] for k in range(side)])
            row[s, 1:2, :] = functools.reduce(jnp.add, [st1[s, k, 1:2, :] for k in range(side)])
            st2[s, y] = row[s]
            start(st2_copy(i))

    def st_all(i):
        s = lax.rem(i, 2)
        st_wait(st2_copy(i), 1)
        full = join([st2[s, k, 0:1, :] for k in range(side)])
        hit = functools.reduce(jnp.add, [st2[s, k, 1:2, :] for k in range(side)])
        lse[0:1, :] = full + math.log2(tokens)
        lossacc[...] += full - hit

    def step(i, carry):
        c = i - 2
        slot = lax.rem(i, 2)
        has_a, has_c = i < chunks, jnp.logical_and(c >= 0, c < chunks)

        @pl.when(i + 1 < chunks)
        def _():
            h_start(i + 1)

        @pl.when(has_a)
        def _():
            h_wait(i)

        @pl.when(jnp.logical_and(has_a, has_c))
        def _():
            two(lambda j: (grad_logits(c, j, slot), logits(i, j, slot)))

        @pl.when(jnp.logical_and(has_a, jnp.logical_not(has_c)))
        def _():
            two(lambda j: logits(i, j, slot))
            two(lambda j: statistics(i, j, slot))

        @pl.when(jnp.logical_and(has_c, jnp.logical_not(has_a)))
        def _():
            two(lambda j: grad_logits(c, j, slot))

        def live(k):
            return jnp.logical_and(k >= 0, k < chunks)

        @pl.when(has_c)
        def _():
            start(dz_copy(c))

        guarded(live(c - 3), lambda: finish(c - 3))
        guarded(live(c - 2), lambda: turn(c - 2))
        guarded(live(c - 1), lambda: start(rs(PURE1, c - 1)))
        later = jnp.logical_and(lax.rem(c, stride) == stride - 1, c // stride < LATER)
        now = jnp.logical_and(jnp.logical_and(c >= 0, c < chunks - 2), jnp.logical_not(later))
        save = jnp.logical_and(jnp.logical_and(c >= 0, c < chunks - 2), later)

        @pl.when(now)
        def _():
            def half_dw(j):
                statistics(i, j, slot)
                grad_w(c, j)

            lax.fori_loop(0, one, lambda j, u: (half_dw(j), u)[1], 0)
            guarded(live(i - 1), lambda: st_row(i - 1))
            lax.fori_loop(one, 2, lambda j, u: (half_dw(j), u)[1], 0)

        @pl.when(jnp.logical_not(now))
        def _():
            @pl.when(save)
            def _():
                pltpu.make_async_copy(dz.at[lax.rem(c + 2, 2)], dz_hbm.at[c // stride], dxsem).start()
                two(lambda j: statistics(i, j, slot))

            guarded(live(i - 1), lambda: st_row(i - 1))

        @pl.when(c == chunks)
        def _():
            two(lambda j: grad_w(c - 2, j))

        guarded(live(c - 1), lambda: merge1(c - 1))
        guarded(live(c - 2), lambda: merge2(c - 2))
        guarded(has_a, lambda: st_own(i))

        @pl.when(has_c)
        def _():
            guarded(c == 0, w_remote.wait_recv)
            wait_recv(dz_copy(c))
            grad_h(c)

        guarded(live(i - 1), lambda: st_all(i - 1))
        guarded(has_a, lambda: st_pair(i))

        @pl.when(has_c)
        def _():
            start(rs(FAR1, c))
            wait_send(dz_copy(c))

        @pl.when(save)
        def _():
            pltpu.make_async_copy(dz.at[lax.rem(c + 2, 2)], dz_hbm.at[c // stride], dxsem).wait()

        @pl.when(c == chunks)
        def _():
            two(lambda j: grad_w(c - 1, j))
            pltpu.make_async_copy(dwacc, dw_hbm, dwsem).start()

        return carry

    lax.fori_loop(0, chunks + 5, step, 0)

    for i in range(max(chunks - 2, 0), chunks):
        guarded(core == 0, lambda: wait_send(st0_copy(i) + st2_copy(i)))
        guarded(core == 1, lambda: wait_send(st1_copy(i)))
        pltpu.make_async_copy(ob.at[i % 2], dh_hbm.at[i], osem.at[i % 2]).wait()
    w_remote.wait_send()
    pltpu.make_async_copy(dwacc, dw_hbm, dwsem).wait()
    loss_ref[...] = jnp.broadcast_to(jnp.sum(lossacc[...], axis=1, keepdims=True) * (LN2 / tokens), loss_ref.shape)


def last_kernel(side, dw_ref, dh_ref, dz_ref, *rest):
    hid, (dw_out, dh_out) = rest[:LATER], rest[LATER:]
    total = dw_ref[...]
    for k in range(LATER):
        h = hid[k]
        by_x = [h[yy, xx, 0, 0] for xx in range(side) for yy in range(side)]
        by_y = [h[yy, xx, 1, 0] for yy in range(side) for xx in range(side)]
        total += dot_nn(dz_ref[k, 0], jnp.concatenate(by_x, axis=0)) + dot_nn(dz_ref[k, 1], jnp.concatenate(by_y, axis=0))
    dw_out[...] = total
    dh_out[...] = dh_ref[...]


def solution(mesh):
    group = mesh.shape[AXIS]
    side = math.isqrt(group // 2)

    def local_step(hidden, targets, w_blk):
        tokens, dim = hidden.shape
        vocab = w_blk.shape[0]
        chunks = tokens // group // ROWS
        tok = group * ROWS
        half = dim // 2
        hid = hidden.reshape(side, side, 2, chunks, ROWS, dim)
        t = targets.reshape(side, side, 2, chunks, ROWS)
        tgt = jnp.concatenate(
            [t[:, :, 0].transpose(2, 1, 0, 3).reshape(chunks, 1, tok // 2), t[:, :, 1].transpose(2, 0, 1, 3).reshape(chunks, 1, tok // 2)],
            axis=2,
        )
        dma = pltpu.SemaphoreType.DMA
        any_spec = pl.BlockSpec(memory_space=pl.ANY)
        vmem_spec = pl.BlockSpec(memory_space=pltpu.VMEM)
        big, small = (2, 2, side * ROWS, half), (2, 2, ROWS, half)
        loss, dh, dw, dz_left = pl.pallas_call(
            functools.partial(head_kernel, group, side, chunks, tokens),
            out_shape=(
                jax.ShapeDtypeStruct((1, 128), F32),
                jax.ShapeDtypeStruct((chunks, ROWS, dim), F32),
                jax.ShapeDtypeStruct((vocab, dim), F32),
                jax.ShapeDtypeStruct((LATER, 2, vocab, tok // 2), BF16),
            ),
            in_specs=[any_spec, vmem_spec, any_spec],
            out_specs=(vmem_spec, any_spec, any_spec, any_spec),
            scratch_shapes=[
                pltpu.VMEM((2, vocab, dim), BF16),
                pltpu.VMEM((vocab, dim), F32),
                pltpu.VMEM((4, 2 * side, side, ROWS, dim), BF16),
                pltpu.VMEM((2, vocab, tok), F32),
                pltpu.VMEM((2, 2, vocab, tok // 2), BF16),
                pltpu.VMEM((2, vocab, tok // 2), BF16),
                pltpu.VMEM((2, side, side * ROWS, dim), F32),
                pltpu.VMEM((2, side, ROWS, dim), F32),
                *[pltpu.VMEM(big, F32)] * 3,
                *[pltpu.VMEM(small, F32)] * 3,
                pltpu.VMEM((2, ROWS, dim), F32),
                pltpu.VMEM((2, 2, tok), F32),
                pltpu.VMEM((2, 2, tok), F32),
                pltpu.VMEM((2, 2, tok), F32),
                pltpu.VMEM((2, 2, tok), F32),
                pltpu.VMEM((2, side, 2, tok), F32),
                pltpu.VMEM((2, 2, tok), F32),
                pltpu.VMEM((2, side, 2, tok), F32),
                pltpu.VMEM((1, tok), F32),
                pltpu.VMEM((1, tok), F32),
                dma, dma((4,)),
                dma((6, 2, 2)), dma((6, 2, 2)),
                dma, dma((2,)), dma, dma,
                dma((2,)), dma((2,)),
                dma((2, 2 * side - 1)), dma((2, side)),
                dma((2, 2 * side - 1)), dma((2, side)),
                dma((2,)), dma, dma,
            ],
            compiler_params=pltpu.CompilerParams(
                collective_id=0, has_side_effects=True, vmem_limit_bytes=67043328,
            ),
            name="head",
        )(hid, tgt, w_blk)
        steps = 8
        stride = chunks // (LATER + 1)
        dw_spec, dh_spec = [pl.BlockSpec((n // steps, dim), lambda j: (j, 0)) for n in (vocab, tokens // group)]
        dz_spec = pl.BlockSpec((LATER, 2, vocab // steps, tok // 2), lambda j: (0, 0, j, 0))
        h_specs = [
            pl.BlockSpec((side, side, 2, 1, ROWS, dim), lambda j, k=k: (0, 0, 0, (k + 1) * stride - 1, 0, 0)) for k in range(LATER)
        ]
        dw, dh = pl.pallas_call(
            functools.partial(last_kernel, side),
            grid=(steps,),
            out_shape=(jax.ShapeDtypeStruct((vocab, dim), F32), jax.ShapeDtypeStruct((tokens // group, dim), F32)),
            in_specs=[dw_spec, dh_spec, dz_spec, *h_specs],
            out_specs=(dw_spec, dh_spec),
            compiler_params=pltpu.CompilerParams(dimension_semantics=("arbitrary",), vmem_limit_bytes=67043328),
            name="last",
        )(dw, dh.reshape(tokens // group, dim), dz_left, *[hid] * LATER)
        return loss[0, :1], dh, dw

    return jax.shard_map(
        local_step,
        mesh=mesh,
        in_specs=(P("data", None), P("data"), P(AXIS, None)),
        out_specs=(P("data"), P(("data", AXIS), None), P(("data", AXIS), None)),
        check_vma=False,
    )
```

```python
import functools
import math

import jax
import jax.numpy as jnp
from jax import lax
from jax.experimental import pallas as pl
from jax.experimental.pallas import tpu as pltpu
from jax.sharding import PartitionSpec as P

F32 = jnp.float32
BF16 = jnp.bfloat16
LOG2E = 1.4426950408889634
LN2 = 0.6931471805599453
ROWS = 16
AXIS = "fsdp"

FAR1, PURE1, MERGED1, FAR2, PURE2, MERGED2 = range(6)


def dot_nt(a, b):
    return lax.dot_general(a, b, (((1,), (1,)), ((), ())), preferred_element_type=F32)


def dot_nn(a, b):
    return lax.dot_general(a, b, (((1,), (0,)), ((), ())), preferred_element_type=F32)


def dot_tn(a, b):
    return lax.dot_general(a, b, (((0,), (0,)), ((), ())), preferred_element_type=F32)


def join(parts):
    top = functools.reduce(jnp.maximum, parts)
    total = functools.reduce(jnp.add, [jnp.exp2(v - top) for v in parts])
    return top + jnp.log(total) * LOG2E


def head_kernel(
    group, side, chunks, tokens,
    hid, tgt, w_hbm,
    loss_ref, dh_hbm, dw_hbm,
    wb, dwacc, hb, yb, dz, dzr, sb, tb, far1, pure1, merged1, far2, pure2, merged2, ob,
    stat, own, st0, mid, st1, row, st2, lse, lossacc,
    wsem, hsem, rs_send, rs_recv, dz_send, dz_recv, w_send, w_recv,
    st0_send, st0_recv, st1_send, st1_recv, st2_send, st2_recv, osem, dwsem,
):
    vocab, dim = w_hbm.shape
    half = dim // 2
    mt = vocab // 2
    tok = hb.shape[1] * hb.shape[2] * ROWS
    tokc = tok // 2

    me = lax.axis_index(AXIS)
    core = lax.rem(me, 2)
    other = 1 - core
    x = lax.rem(me // 2, side)
    y = me // (2 * side)
    p = x + core * (y - x)
    q = y + core * (x - y)
    partner = me + 1 - 2 * core
    one = 1 + me // group

    def at_xy(xx, yy):
        return (lax.rem(yy + side, side) * side + lax.rem(xx + side, side)) * 2 + core

    def at_pq(pp, qq):
        return at_xy(pp + core * (qq - pp), qq + core * (pp - qq))

    peers_x = [at_xy(x + k, y) for k in range(1, side)]
    peers_y = [at_xy(x, y + k) for k in range(1, side)]
    to_p, to_q = (at_pq(p + 1, q), at_pq(p - 1, q)), (at_pq(p, q + 1), at_pq(p, q - 1))
    near_p = lax.rem(p + 1, side), lax.rem(p + side - 1, side), lax.rem(p + 2, side)
    near_q = lax.rem(q + 1, side), lax.rem(q + side - 1, side), lax.rem(q + 2, side)

    def rcopy(src, dst, send, recv, dev):
        return pltpu.make_async_remote_copy(
            src_ref=src, dst_ref=dst, send_sem=send, recv_sem=recv,
            device_id={AXIS: dev}, device_id_type=pl.DeviceIdType.MESH,
        )

    steady = [False]

    def guarded(cond, fn):
        if steady[0]:
            fn()
        else:
            pl.when(cond)(lambda: (fn(), None)[1])

    def both_ways(cond, fn):
        @pl.when(cond)
        def _():
            steady[0] = True
            fn()
            steady[0] = False

        pl.when(jnp.logical_not(cond))(fn)

    barrier = pltpu.get_barrier_semaphore()
    friends = [partner] + [peer + o for peer in (*peers_x, *peers_y) for o in (0, 1 - 2 * core)]
    for dev in friends:
        pl.semaphore_signal(barrier, inc=1, device_id={AXIS: dev}, device_id_type=pl.DeviceIdType.MESH)

    def h_copies(c):
        s = lax.rem(c, 4)
        out = []
        for k in range(side):
            out.append(pltpu.make_async_copy(hid.at[:, k, 0, c], hb.at[s, k], hsem.at[s]))
            out.append(pltpu.make_async_copy(hid.at[k, :, 1, c], hb.at[s, side + k], hsem.at[s]))
        return out

    def h_start(c):
        for d in h_copies(c):
            d.start()

    def h_wait(c):
        s = lax.rem(c, 4)
        pltpu.make_async_copy(hb.at[s], hb.at[s], hsem.at[s]).wait()

    w_local = pltpu.make_async_copy(w_hbm, wb.at[core], wsem)
    w_local.start()
    h_start(0)
    dwacc[...] = jnp.zeros_like(dwacc)
    lossacc[...] = jnp.zeros_like(lossacc)
    pl.semaphore_wait(barrier, len(friends))
    w_local.wait()
    w_remote = rcopy(wb.at[core], wb.at[core], w_send, w_recv, partner)
    w_remote.start()

    def rs(kind, c):
        s = t = lax.rem(c, 2)
        if kind >= FAR2:
            t = lax.rem(c, 3)
        lo, hi = pl.ds(0, half), pl.ds(half, half)
        buf, to, (up, down, far) = (sb, to_p, near_p) if kind < 3 else (tb, to_q, near_q)
        dst = (far1, pure1, merged1, far2, pure2, merged2)[kind]
        src = {0: ((far, lo), (far, hi)), 1: ((up, hi), (down, lo)), 2: ((up, lo), (down, hi))}[kind % 3]
        return [
            rcopy(buf.at[s, src[d][0], :, src[d][1]], dst.at[t, d], rs_send.at[kind, t, d], rs_recv.at[kind, t, d], to[d])
            for d in range(2)
        ]

    def start(ds):
        for d in ds:
            d.start()

    def wait_recv(ds):
        for d in ds:
            d.wait_recv()

    def wait_send(ds):
        for d in ds:
            d.wait_send()

    def dz_copy(c):
        s = lax.rem(c, 2)
        return [rcopy(dz.at[s, other], dzr.at[s], dz_send, dz_recv.at[s], partner)]

    def st0_copy(i):
        s = lax.rem(i, 2)
        return [rcopy(own.at[s], st0.at[s], st0_send.at[s], st0_recv.at[s], partner)]

    def st1_copy(i):
        s = lax.rem(i, 2)
        to = [(peer - o, k) for k, peer in enumerate(peers_x) for o in (0, 1)] + [(partner, side - 1)]
        return [rcopy(mid.at[s], st1.at[s, x], st1_send.at[s, n], st1_recv.at[s, k], dev) for n, (dev, k) in enumerate(to)]

    def st2_copy(i):
        s = lax.rem(i, 2)
        to = [(peer + o, k) for k, peer in enumerate(peers_y) for o in (0, 1)] + [(partner, side - 1)]
        return [rcopy(row.at[s], st2.at[s, y], st2_send.at[s, n], st2_recv.at[s, k], dev) for n, (dev, k) in enumerate(to)]

    def st_wait(copies, partner_core):
        wait_recv(copies[0:-1:2])
        pl.when(core == partner_core)(lambda: wait_recv(copies[-1:]))

    def two(fn):
        lax.fori_loop(0, 2, lambda j, carry: (fn(j), carry)[1], 0)

    def logits(i, j, slot):
        r = pl.ds(pl.multiple_of(j * mt, mt), mt)
        h = hb[lax.rem(i, 4)].reshape(tok, dim)
        yb[slot, r, :] = dot_nt(wb[core, r, :], h) * LOG2E

    def grad_logits(c, j, slot):
        r = pl.ds(pl.multiple_of(j * mt, mt), mt)
        prob = jnp.exp2(yb[slot, r, :] - lse[0:1, :])
        hit = lax.broadcasted_iota(jnp.int32, prob.shape, 0) == tgt[c] - (me * vocab + j * mt)
        g = (prob + jnp.where(hit, -1.0 / tokens, 0.0)).astype(BF16)
        dz[slot, 0, r, :] = g[:, :tokc]
        dz[slot, 1, r, :] = g[:, tokc:]

    def statistics(i, j, slot):
        v = yb[slot, pl.ds(pl.multiple_of(j * mt, mt), mt), :]
        top = jnp.max(v, axis=0, keepdims=True)
        total = jnp.sum(jnp.exp2(v - top), axis=0, keepdims=True)
        hit = lax.broadcasted_iota(jnp.int32, v.shape, 0) == tgt[lax.rem(i, chunks)] - (me * vocab + j * mt)
        stat[j, 0:1, :] = top + jnp.log(total) * LOG2E
        stat[j, 1:2, :] = jnp.sum(jnp.where(hit, v, 0.0), axis=0, keepdims=True)

    def grad_w(c, k):
        n = dim // 2
        cols = pl.ds(pl.multiple_of(k * n, n), n)
        h = hb[lax.rem(c, 4), :, :, :, cols].reshape(tok, n)
        s = lax.rem(c, 2)
        dwacc[:, cols] += dot_nn(dz[s, 0], h[:tokc]) + dot_nn(dz[s, 1], h[tokc:])

    def grad_h(c):
        s = lax.rem(c, 2)
        v = dot_tn(dz[s, core], wb[core]) + dot_tn(dzr[s], wb[other])
        sb[s] = v.reshape(side, side * ROWS, dim)

    def finish(c):
        s = lax.rem(c, 2)
        wait_recv(rs(PURE2, c) + rs(MERGED2, c))
        wait_send(rs(FAR2, c) + rs(PURE2, c) + rs(MERGED2, c))
        guarded(c >= 2, lambda: pltpu.make_async_copy(ob.at[s], dh_hbm.at[c - 2], osem.at[s]).wait())
        t = lax.rem(c, 3)
        ob[s, :, :half] = tb[s, q, :, :half] + merged2[t, 0] + pure2[t, 1]
        ob[s, :, half:] = tb[s, q, :, half:] + pure2[t, 0] + merged2[t, 1]
        pltpu.make_async_copy(ob.at[s], dh_hbm.at[c], osem.at[s]).start()

    def turn(c):
        s = lax.rem(c, 2)
        wait_recv(rs(PURE1, c) + rs(MERGED1, c))
        lo = sb[s, p, :, :half] + merged1[s, 0] + pure1[s, 1]
        hi = sb[s, p, :, half:] + pure1[s, 0] + merged1[s, 1]
        tb[s, :, :, :half] = lo.reshape(side, ROWS, half)
        tb[s, :, :, half:] = hi.reshape(side, ROWS, half)
        start(rs(FAR2, c) + rs(PURE2, c))
        wait_send(rs(FAR1, c) + rs(PURE1, c) + rs(MERGED1, c))

    def merge1(c):
        s = lax.rem(c, 2)
        up, down, _ = near_p
        wait_recv(rs(FAR1, c))
        sb[s, up, :, :half] += far1[s, 0]
        sb[s, down, :, half:] += far1[s, 1]
        start(rs(MERGED1, c))

    def merge2(c):
        s = lax.rem(c, 2)
        up, down, _ = near_q
        wait_recv(rs(FAR2, c))
        t = lax.rem(c, 3)
        tb[s, up, :, :half] += far2[t, 0]
        tb[s, down, :, half:] += far2[t, 1]
        start(rs(MERGED2, c))

    def st_own(i):
        s = lax.rem(i, 2)

        @pl.when(core == 0)
        def _():
            guarded(i >= 2, lambda: wait_send(st0_copy(i)))

        own[s, 0:1, :] = join([stat[0, 0:1, :], stat[1, 0:1, :]])
        own[s, 1:2, :] = stat[0, 1:2, :] + stat[1, 1:2, :]
        pl.when(core == 0)(lambda: start(st0_copy(i)))

    def st_pair(i):
        s = lax.rem(i, 2)

        @pl.when(core == 1)
        def _():
            wait_recv(st0_copy(i))
            guarded(i >= 2, lambda: wait_send(st1_copy(i)))
            mid[s, 0:1, :] = join([st0[s, 0:1, :], own[s, 0:1, :]])
            mid[s, 1:2, :] = st0[s, 1:2, :] + own[s, 1:2, :]
            start(st1_copy(i))

    def st_row(i):
        s = lax.rem(i, 2)
        st_wait(st1_copy(i), 0)

        @pl.when(core == 0)
        def _():
            guarded(i >= 2, lambda: wait_send(st2_copy(i)))
            row[s, 0:1, :] = join([st1[s, k, 0:1, :] for k in range(side)])
            row[s, 1:2, :] = functools.reduce(jnp.add, [st1[s, k, 1:2, :] for k in range(side)])
            st2[s, y] = row[s]
            start(st2_copy(i))

    def st_all(i):
        s = lax.rem(i, 2)
        st_wait(st2_copy(i), 1)
        full = join([st2[s, k, 0:1, :] for k in range(side)])
        hit = functools.reduce(jnp.add, [st2[s, k, 1:2, :] for k in range(side)])
        lse[0:1, :] = full + math.log2(tokens)
        lossacc[...] += full - hit

    def step(i, carry):
        c = i - 2
        slot = lax.rem(i, 2)
        has_a, has_c = i < chunks, jnp.logical_and(c >= 0, c < chunks)

        @pl.when(i + 1 < chunks)
        def _():
            h_start(i + 1)

        @pl.when(has_a)
        def _():
            h_wait(i)

        @pl.when(jnp.logical_and(has_a, has_c))
        def _():
            two(lambda j: (grad_logits(c, j, slot), logits(i, j, slot)))

        @pl.when(jnp.logical_and(has_a, jnp.logical_not(has_c)))
        def _():
            two(lambda j: logits(i, j, slot))
            two(lambda j: statistics(i, j, slot))

        @pl.when(jnp.logical_and(has_c, jnp.logical_not(has_a)))
        def _():
            two(lambda j: grad_logits(c, j, slot))

        def live(k):
            return jnp.logical_and(k >= 0, k < chunks)

        def live(k):
            return jnp.logical_and(k >= 0, k < chunks)

        calm = jnp.logical_and(i >= 7, i < chunks)

        def point_a():
            guarded(has_c, lambda: start(dz_copy(c)))
            guarded(live(c - 2), lambda: turn(c - 2))
            guarded(live(c - 1), lambda: start(rs(PURE1, c - 1)))

        def point_m():
            guarded(live(c - 1), lambda: merge1(c - 1))
            guarded(has_a, lambda: st_own(i))
            guarded(live(c - 3), lambda: finish(c - 3))

        def point_b():
            guarded(live(i - 1), lambda: st_all(i - 1))
            guarded(has_a, lambda: st_pair(i))
            guarded(has_c, lambda: (start(rs(FAR1, c)), wait_send(dz_copy(c))))
            guarded(live(c - 2), lambda: merge2(c - 2))

        both_ways(calm, point_a)

        now = jnp.logical_and(c >= 0, c < chunks - 2)

        @pl.when(now)
        def _():
            def half_dw(j):
                statistics(i, j, slot)
                grad_w(c, j)

            lax.fori_loop(0, one, lambda j, u: (half_dw(j), u)[1], 0)
            both_ways(calm, lambda: guarded(live(i - 1), lambda: st_row(i - 1)))
            lax.fori_loop(one, 2, lambda j, u: (half_dw(j), u)[1], 0)

        pl.when(jnp.logical_and(jnp.logical_not(now), live(i - 1)))(lambda: st_row(i - 1))

        @pl.when(c == chunks)
        def _():
            two(lambda j: grad_w(c - 2, j))

        both_ways(calm, point_m)

        @pl.when(has_c)
        def _():
            pl.when(c == 0)(w_remote.wait_recv)
            wait_recv(dz_copy(c))
            grad_h(c)

        both_ways(calm, point_b)

        @pl.when(c == chunks)
        def _():
            two(lambda j: grad_w(c - 1, j))
            pltpu.make_async_copy(dwacc, dw_hbm, dwsem).start()

        return carry

    lax.fori_loop(0, chunks + 5, step, 0)

    for i in range(max(chunks - 2, 0), chunks):
        guarded(core == 0, lambda: wait_send(st0_copy(i) + st2_copy(i)))
        guarded(core == 1, lambda: wait_send(st1_copy(i)))
        pltpu.make_async_copy(ob.at[i % 2], dh_hbm.at[i], osem.at[i % 2]).wait()
    w_remote.wait_send()
    pltpu.make_async_copy(dwacc, dw_hbm, dwsem).wait()
    loss_ref[...] = jnp.broadcast_to(jnp.sum(lossacc[...], axis=1, keepdims=True) * (LN2 / tokens), loss_ref.shape)


def copy_kernel(dw_hbm, dh_hbm, dw_out, dh_out, buf, isem, osem):
    rows = buf.shape[1]
    pieces = [(src.at[pl.ds(r, rows)], dst.at[pl.ds(r, rows)]) for src, dst in ((dw_hbm, dw_out), (dh_hbm, dh_out)) for r in range(0, src.shape[0], rows)]
    get = [pltpu.make_async_copy(src, buf.at[k], isem.at[k]) for k, (src, _) in enumerate(pieces)]
    put = [pltpu.make_async_copy(buf.at[k], dst, osem.at[k]) for k, (_, dst) in enumerate(pieces)]
    for copy in get:
        copy.start()
    for copy, back in zip(get, put):
        copy.wait()
        back.start()
    for back in put:
        back.wait()


def solution(mesh):
    group = mesh.shape[AXIS]
    side = math.isqrt(group // 2)

    def local_step(hidden, targets, w_blk):
        tokens, dim = hidden.shape
        vocab = w_blk.shape[0]
        chunks = tokens // group // ROWS
        tok = group * ROWS
        half = dim // 2
        hid = hidden.reshape(side, side, 2, chunks, ROWS, dim)
        t = targets.reshape(side, side, 2, chunks, ROWS)
        tgt = jnp.concatenate(
            [t[:, :, 0].transpose(2, 1, 0, 3).reshape(chunks, 1, tok // 2), t[:, :, 1].transpose(2, 0, 1, 3).reshape(chunks, 1, tok // 2)],
            axis=2,
        )
        dma = pltpu.SemaphoreType.DMA
        any_spec = pl.BlockSpec(memory_space=pl.ANY)
        vmem_spec = pl.BlockSpec(memory_space=pltpu.VMEM)
        big, small = (2, 2, side * ROWS, half), (3, 2, ROWS, half)
        loss, dh, dw = pl.pallas_call(
            functools.partial(head_kernel, group, side, chunks, tokens),
            out_shape=(
                jax.ShapeDtypeStruct((1, 128), F32),
                jax.ShapeDtypeStruct((chunks, ROWS, dim), F32),
                jax.ShapeDtypeStruct((vocab, dim), F32),
            ),
            in_specs=[any_spec, vmem_spec, any_spec],
            out_specs=(vmem_spec, any_spec, any_spec),
            scratch_shapes=[
                pltpu.VMEM((2, vocab, dim), BF16),
                pltpu.VMEM((vocab, dim), F32),
                pltpu.VMEM((4, 2 * side, side, ROWS, dim), BF16),
                pltpu.VMEM((2, vocab, tok), F32),
                pltpu.VMEM((2, 2, vocab, tok // 2), BF16),
                pltpu.VMEM((2, vocab, tok // 2), BF16),
                pltpu.VMEM((2, side, side * ROWS, dim), F32),
                pltpu.VMEM((2, side, ROWS, dim), F32),
                *[pltpu.VMEM(big, F32)] * 3,
                *[pltpu.VMEM(small, F32)] * 3,
                pltpu.VMEM((2, ROWS, dim), F32),
                pltpu.VMEM((2, 2, tok), F32),
                pltpu.VMEM((2, 2, tok), F32),
                pltpu.VMEM((2, 2, tok), F32),
                pltpu.VMEM((2, 2, tok), F32),
                pltpu.VMEM((2, side, 2, tok), F32),
                pltpu.VMEM((2, 2, tok), F32),
                pltpu.VMEM((2, side, 2, tok), F32),
                pltpu.VMEM((1, tok), F32),
                pltpu.VMEM((1, tok), F32),
                dma, dma((4,)),
                dma((6, 3, 2)), dma((6, 3, 2)),
                dma, dma((2,)), dma, dma,
                dma((2,)), dma((2,)),
                dma((2, 2 * side - 1)), dma((2, side)),
                dma((2, 2 * side - 1)), dma((2, side)),
                dma((2,)), dma,
            ],
            compiler_params=pltpu.CompilerParams(
                collective_id=0, has_side_effects=True, vmem_limit_bytes=67043328,
            ),
            name="head",
        )(hid, tgt, w_blk)
        rows = tokens // group // 4
        pieces = (vocab + tokens // group) // rows
        dw, dh = pl.pallas_call(
            copy_kernel,
            out_shape=(jax.ShapeDtypeStruct((vocab, dim), F32), jax.ShapeDtypeStruct((tokens // group, dim), F32)),
            in_specs=[any_spec] * 2,
            out_specs=(any_spec, any_spec),
            scratch_shapes=[pltpu.VMEM((pieces, rows, dim), F32), dma((pieces,)), dma((pieces,))],
            compiler_params=pltpu.CompilerParams(vmem_limit_bytes=67043328),
            name="results",
        )(dw, dh.reshape(tokens // group, dim))
        return loss[0, :1], dh, dw

    return jax.shard_map(
        local_step,
        mesh=mesh,
        in_specs=(P("data", None), P("data"), P(AXIS, None)),
        out_specs=(P("data"), P(("data", AXIS), None), P(("data", AXIS), None)),
        check_vma=False,
    )
```

```python
import functools
import math

import jax
import jax.numpy as jnp
from jax import lax
from jax.experimental import pallas as pl
from jax.experimental.pallas import tpu as pltpu
from jax.sharding import PartitionSpec as P

F32 = jnp.float32
BF16 = jnp.bfloat16
LOG2E = 1.4426950408889634
LN2 = 0.6931471805599453
LATE = 2
ROWS = 16
AXIS = "fsdp"

FAR1, PURE1, MERGED1, FAR2, PURE2, MERGED2 = range(6)


def dot_nt(a, b):
    return lax.dot_general(a, b, (((1,), (1,)), ((), ())), preferred_element_type=F32)


def dot_nn(a, b):
    return lax.dot_general(a, b, (((1,), (0,)), ((), ())), preferred_element_type=F32)


def dot_tn(a, b):
    return lax.dot_general(a, b, (((0,), (0,)), ((), ())), preferred_element_type=F32)


def join(parts):
    top = functools.reduce(jnp.maximum, parts)
    total = functools.reduce(jnp.add, [jnp.exp2(v - top) for v in parts])
    return top + jnp.log(total) * LOG2E


class Chunk:
    def __init__(self, n, two, three):
        self.n, self.two, self.three = n, two, three


def head_kernel(
    group, side, chunks, tokens,
    hid, tgt, w_hbm,
    loss_ref, dh_hbm, dw_hbm,
    wb, dwacc, hb, yb, dz, dzr, sb, tb, far1, pure1, merged1, far2, pure2, merged2, ob,
    stat, own, st0, mid, st1, row, st2, lse, lossacc,
    wsem, hsem, rs_send, rs_recv, dz_send, dz_recv, w_send, w_recv,
    st0_send, st0_recv, st1_send, st1_recv, st2_send, st2_recv, osem, dwsem,
):
    vocab, dim = w_hbm.shape
    half = dim // 2
    mt = vocab // 2
    tok = hb.shape[1] * hb.shape[2] * ROWS
    tokc = tok // 2

    me = lax.axis_index(AXIS)
    core = lax.rem(me, 2)
    other = 1 - core
    x = lax.rem(me // 2, side)
    y = me // (2 * side)
    p = x + core * (y - x)
    q = y + core * (x - y)
    partner = me + 1 - 2 * core
    one = 1 + me // group

    def at_xy(xx, yy):
        return (lax.rem(yy + side, side) * side + lax.rem(xx + side, side)) * 2 + core

    def at_pq(pp, qq):
        return at_xy(pp + core * (qq - pp), qq + core * (pp - qq))

    peers_x = [at_xy(x + k, y) for k in range(1, side)]
    peers_y = [at_xy(x, y + k) for k in range(1, side)]
    to_p, to_q = (at_pq(p + 1, q), at_pq(p - 1, q)), (at_pq(p, q + 1), at_pq(p, q - 1))
    near_p = lax.rem(p + 1, side), lax.rem(p + side - 1, side), lax.rem(p + 2, side)
    near_q = lax.rem(q + 1, side), lax.rem(q + side - 1, side), lax.rem(q + 2, side)

    def rcopy(src, dst, send, recv, dev):
        return pltpu.make_async_remote_copy(
            src_ref=src, dst_ref=dst, send_sem=send, recv_sem=recv,
            device_id={AXIS: dev}, device_id_type=pl.DeviceIdType.MESH,
        )

    steady = [False]

    def guarded(cond, fn):
        if steady[0]:
            fn()
        else:
            pl.when(cond)(lambda: (fn(), None)[1])

    def both_ways(cond, fn):
        @pl.when(cond)
        def _():
            steady[0] = True
            fn()
            steady[0] = False

        pl.when(jnp.logical_not(cond))(fn)

    barrier = pltpu.get_barrier_semaphore()
    friends = [partner] + [peer + o for peer in (*peers_x, *peers_y) for o in (0, 1 - 2 * core)]
    for dev in friends:
        pl.semaphore_signal(barrier, inc=1, device_id={AXIS: dev}, device_id_type=pl.DeviceIdType.MESH)

    def h_start(n, s):
        for k in range(side):
            pltpu.make_async_copy(hid.at[:, k, 0, n], hb.at[s, k], hsem.at[s]).start()
            pltpu.make_async_copy(hid.at[k, :, 1, n], hb.at[s, side + k], hsem.at[s]).start()

    def h_wait(s):
        pltpu.make_async_copy(hb.at[s], hb.at[s], hsem.at[s]).wait()

    w_local = [
        pltpu.make_async_copy(w_hbm.at[pl.ds(k * mt, mt)], wb.at[core, pl.ds(k * mt, mt)], wsem.at[k]) for k in range(2)
    ]
    w_local[0].start()
    h_start(0, 0)
    w_local[1].start()
    dwacc[...] = jnp.zeros_like(dwacc)
    lossacc[...] = jnp.zeros_like(lossacc)
    w_local[0].wait()
    w_remote = rcopy(wb.at[core], wb.at[core], w_send, w_recv, partner)

    def rs(kind, c):
        s, t = c.two, c.three if kind >= FAR2 else c.two
        lo, hi = pl.ds(0, half), pl.ds(half, half)
        buf, to, (up, down, far) = (sb, to_p, near_p) if kind < 3 else (tb, to_q, near_q)
        dst = (far1, pure1, merged1, far2, pure2, merged2)[kind]
        src = {0: ((far, lo), (far, hi)), 1: ((up, hi), (down, lo)), 2: ((up, lo), (down, hi))}[kind % 3]
        return [
            rcopy(buf.at[s, src[d][0], :, src[d][1]], dst.at[t, d], rs_send.at[kind, t, d], rs_recv.at[kind, t, d], to[d])
            for d in range(2)
        ]

    def start(ds):
        for d in ds:
            d.start()

    def wait_recv(ds):
        for d in ds:
            d.wait_recv()

    def wait_send(ds):
        for d in ds:
            d.wait_send()

    def dz_copy(c):
        return [rcopy(dz.at[c.three, other], dzr.at[c.two], dz_send, dz_recv.at[c.two], partner)]

    def st0_copy(c):
        s = c.two
        return [rcopy(own.at[s], st0.at[s], st0_send.at[s], st0_recv.at[s], partner)]

    def st1_copy(c):
        s = c.two
        to = [(peer - o, k) for k, peer in enumerate(peers_x) for o in (0, 1)] + [(partner, side - 1)]
        return [rcopy(mid.at[s], st1.at[s, x], st1_send.at[s, n], st1_recv.at[s, k], dev) for n, (dev, k) in enumerate(to)]

    def st2_copy(c):
        s = c.two
        to = [(peer + o, k) for k, peer in enumerate(peers_y) for o in (0, 1)] + [(partner, side - 1)]
        return [rcopy(row.at[s], st2.at[s, y], st2_send.at[s, n], st2_recv.at[s, k], dev) for n, (dev, k) in enumerate(to)]

    def st_wait(copies, partner_core):
        wait_recv(copies[0:-1:2])
        pl.when(core == partner_core)(lambda: wait_recv(copies[-1:]))

    def two(fn):
        lax.fori_loop(0, 2, lambda j, carry: (fn(j), carry)[1], 0)

    def logits(c, j):
        r = pl.ds(pl.multiple_of(j * mt, mt), mt)
        h = hb[c.two].reshape(tok, dim)
        yb[c.two, r, :] = dot_nt(wb[core, r, :], h) * LOG2E

    def grad_logits(c, j):
        r = pl.ds(pl.multiple_of(j * mt, mt), mt)
        prob = jnp.exp2(yb[c.two, r, :] - lse[0:1, :])
        hit = lax.broadcasted_iota(jnp.int32, prob.shape, 0) == tgt[c.n] - (me * vocab + j * mt)
        g = (prob + jnp.where(hit, -1.0 / tokens, 0.0)).astype(BF16)
        dz[c.three, 0, r, :] = g[:, :tokc]
        dz[c.three, 1, r, :] = g[:, tokc:]

    def statistics(c, j):
        v = yb[c.two, pl.ds(pl.multiple_of(j * mt, mt), mt), :]
        top = jnp.max(v, axis=0, keepdims=True)
        total = jnp.sum(jnp.exp2(v - top), axis=0, keepdims=True)
        hit = lax.broadcasted_iota(jnp.int32, v.shape, 0) == tgt[lax.rem(c.n, chunks)] - (me * vocab + j * mt)
        stat[j, 0:1, :] = top + jnp.log(total) * LOG2E
        stat[j, 1:2, :] = jnp.sum(jnp.where(hit, v, 0.0), axis=0, keepdims=True)

    def grad_w(c, k):
        n = dim // 2
        cols = pl.ds(pl.multiple_of(k * n, n), n)
        h = hb[2 + c.two, :, :, :, cols].reshape(tok, n)
        dwacc[:, cols] += dot_nn(dz[c.three, 0], h[:tokc]) + dot_nn(dz[c.three, 1], h[tokc:])

    def grad_h(c):
        v = dot_tn(dz[c.three, core], wb[core]) + dot_tn(dzr[c.two], wb[other])
        sb[c.two] = v.reshape(side, side * ROWS, dim)

    def finish(c):
        s, t = c.two, c.three
        wait_recv(rs(PURE2, c) + rs(MERGED2, c))
        wait_send(rs(FAR2, c) + rs(PURE2, c) + rs(MERGED2, c))
        guarded(c.n >= 2, lambda: pltpu.make_async_copy(ob.at[s], dh_hbm.at[c.n - 2], osem.at[s]).wait())
        ob[s, :, :half] = tb[s, q, :, :half] + merged2[t, 0] + pure2[t, 1]
        ob[s, :, half:] = tb[s, q, :, half:] + pure2[t, 0] + merged2[t, 1]
        pltpu.make_async_copy(ob.at[s], dh_hbm.at[c.n], osem.at[s]).start()

    def turn(c):
        s = c.two
        wait_recv(rs(PURE1, c) + rs(MERGED1, c))
        lo = sb[s, p, :, :half] + merged1[s, 0] + pure1[s, 1]
        hi = sb[s, p, :, half:] + pure1[s, 0] + merged1[s, 1]
        tb[s, :, :, :half] = lo.reshape(side, ROWS, half)
        tb[s, :, :, half:] = hi.reshape(side, ROWS, half)
        start(rs(FAR2, c) + rs(PURE2, c))
        wait_send(rs(FAR1, c) + rs(PURE1, c) + rs(MERGED1, c))

    def merge1(c):
        s = c.two
        up, down, _ = near_p
        wait_recv(rs(FAR1, c))
        sb[s, up, :, :half] += far1[s, 0]
        sb[s, down, :, half:] += far1[s, 1]
        start(rs(MERGED1, c))

    def merge2(c):
        s, t = c.two, c.three
        up, down, _ = near_q
        wait_recv(rs(FAR2, c))
        tb[s, up, :, :half] += far2[t, 0]
        tb[s, down, :, half:] += far2[t, 1]
        start(rs(MERGED2, c))

    def st_own(c):
        s = c.two

        @pl.when(core == 0)
        def _():
            guarded(c.n >= 2, lambda: wait_send(st0_copy(c)))

        own[s, 0:1, :] = join([stat[0, 0:1, :], stat[1, 0:1, :]])
        own[s, 1:2, :] = stat[0, 1:2, :] + stat[1, 1:2, :]
        pl.when(core == 0)(lambda: start(st0_copy(c)))

    def st_pair(c):
        s = c.two

        @pl.when(core == 1)
        def _():
            wait_recv(st0_copy(c))
            guarded(c.n >= 2, lambda: wait_send(st1_copy(c)))
            mid[s, 0:1, :] = join([st0[s, 0:1, :], own[s, 0:1, :]])
            mid[s, 1:2, :] = st0[s, 1:2, :] + own[s, 1:2, :]
            start(st1_copy(c))

    def st_row(c):
        s = c.two
        st_wait(st1_copy(c), 0)

        @pl.when(core == 0)
        def _():
            guarded(c.n >= 2, lambda: wait_send(st2_copy(c)))
            row[s, 0:1, :] = join([st1[s, k, 0:1, :] for k in range(side)])
            row[s, 1:2, :] = functools.reduce(jnp.add, [st1[s, k, 1:2, :] for k in range(side)])
            st2[s, y] = row[s]
            start(st2_copy(c))

    def st_all(c):
        s = c.two
        st_wait(st2_copy(c), 1)
        full = join([st2[s, k, 0:1, :] for k in range(side)])
        hit = functools.reduce(jnp.add, [st2[s, k, 1:2, :] for k in range(side)])
        lse[0:1, :] = full + math.log2(tokens)
        lossacc[...] += full - hit

    def chunk(i, k):
        return Chunk(i - k, lax.rem(i + 8 - k, 2), lax.rem(i + 9 - k, 3))

    def step(i, carry):
        ch = [chunk(i, k) for k in range(6)]
        has = [jnp.logical_and(c.n >= 0, c.n < chunks) for c in ch]
        has_a, has_c = has[0], has[2]
        ch[2].two = ch[0].two
        calm = jnp.logical_and(i >= 7, i < chunks)

        @pl.when(i + 1 < chunks)
        def _():
            h_start(i + 1, ch[1].two)

        coming = ch[1 + LATE]

        @pl.when(jnp.logical_and(coming.n >= 0, coming.n < chunks))
        def _():
            h_start(coming.n, 2 + coming.two)

        @pl.when(has_a)
        def _():
            h_wait(ch[0].two)

        @pl.when(jnp.logical_and(has_a, has_c))
        def _():
            two(lambda j: (grad_logits(ch[2], j), logits(ch[0], j)))

        @pl.when(jnp.logical_and(has_a, jnp.logical_not(has_c)))
        def _():
            def first(j):
                pl.when(jnp.logical_and(i == 0, j == 1))(w_local[1].wait)
                logits(ch[0], j)

            two(first)
            two(lambda j: statistics(ch[0], j))

        @pl.when(i == 0)
        def _():
            pl.semaphore_wait(barrier, len(friends))
            w_remote.start()

        @pl.when(jnp.logical_and(has_c, jnp.logical_not(has_a)))
        def _():
            two(lambda j: grad_logits(ch[2], j))

        def point_a():
            guarded(has_c, lambda: start(dz_copy(ch[2])))
            guarded(has[4], lambda: turn(ch[4]))
            guarded(has[3], lambda: start(rs(PURE1, ch[3])))

        def point_m():
            guarded(has[3], lambda: merge1(ch[3]))
            guarded(has_a, lambda: st_own(ch[0]))
            guarded(has[5], lambda: finish(ch[5]))

        def point_b():
            guarded(has[1], lambda: st_all(ch[1]))
            guarded(has_a, lambda: st_pair(ch[0]))
            guarded(has_c, lambda: (start(rs(FAR1, ch[2])), wait_send(dz_copy(ch[2]))))
            guarded(has[4], lambda: merge2(ch[4]))

        both_ways(calm, point_a)

        late = ch[2 + LATE]
        with_statistics = jnp.logical_and(has_a, late.n >= 0)

        @pl.when(jnp.logical_and(late.n >= 0, late.n < chunks - 1))
        def _():
            h_wait(2 + late.two)

        @pl.when(with_statistics)
        def _():
            def half_dw(j):
                statistics(ch[0], j)
                grad_w(late, j)

            lax.fori_loop(0, one, lambda j, u: (half_dw(j), u)[1], 0)
            both_ways(calm, lambda: guarded(has[1], lambda: st_row(ch[1])))
            lax.fori_loop(one, 2, lambda j, u: (half_dw(j), u)[1], 0)

        @pl.when(jnp.logical_not(with_statistics))
        def _():
            pl.when(jnp.logical_and(has_a, has_c))(lambda: two(lambda j: statistics(ch[0], j)))
            pl.when(has[1])(lambda: st_row(ch[1]))
            pl.when(jnp.logical_and(i >= chunks, i < chunks + 3))(lambda: two(lambda j: grad_w(late, j)))

        both_ways(calm, point_m)

        @pl.when(has_c)
        def _():
            pl.when(i == 2)(w_remote.wait_recv)
            wait_recv(dz_copy(ch[2]))
            grad_h(ch[2])

        both_ways(calm, point_b)

        @pl.when(i == chunks + 2)
        def _():
            h_wait(2 + coming.two)
            two(lambda j: grad_w(coming, j))
            pltpu.make_async_copy(dwacc, dw_hbm, dwsem).start()

        return carry

    lax.fori_loop(0, chunks + 5, step, 0)

    for i in range(max(chunks - 2, 0), chunks):
        c = Chunk(i, i % 2, i % 3)
        guarded(core == 0, lambda: wait_send(st0_copy(c) + st2_copy(c)))
        guarded(core == 1, lambda: wait_send(st1_copy(c)))
        pltpu.make_async_copy(ob.at[i % 2], dh_hbm.at[i], osem.at[i % 2]).wait()
    w_remote.wait_send()
    pltpu.make_async_copy(dwacc, dw_hbm, dwsem).wait()
    loss_ref[...] = jnp.broadcast_to(jnp.sum(lossacc[...], axis=1, keepdims=True) * (LN2 / tokens), loss_ref.shape)


def copy_kernel(dw_hbm, dh_hbm, dw_out, dh_out, buf, isem, osem):
    rows = buf.shape[1]
    pieces = [(src.at[pl.ds(r, rows)], dst.at[pl.ds(r, rows)]) for src, dst in ((dw_hbm, dw_out), (dh_hbm, dh_out)) for r in range(0, src.shape[0], rows)]
    get = [pltpu.make_async_copy(src, buf.at[k], isem.at[k]) for k, (src, _) in enumerate(pieces)]
    put = [pltpu.make_async_copy(buf.at[k], dst, osem.at[k]) for k, (_, dst) in enumerate(pieces)]
    for copy in get:
        copy.start()
    for copy, back in zip(get, put):
        copy.wait()
        back.start()
    for back in put:
        back.wait()


def solution(mesh):
    group = mesh.shape[AXIS]
    side = math.isqrt(group // 2)

    def local_step(hidden, targets, w_blk):
        tokens, dim = hidden.shape
        vocab = w_blk.shape[0]
        chunks = tokens // group // ROWS
        tok = group * ROWS
        half = dim // 2
        hid = hidden.reshape(side, side, 2, chunks, ROWS, dim)
        t = targets.reshape(side, side, 2, chunks, ROWS)
        tgt = jnp.concatenate(
            [t[:, :, 0].transpose(2, 1, 0, 3).reshape(chunks, 1, tok // 2), t[:, :, 1].transpose(2, 0, 1, 3).reshape(chunks, 1, tok // 2)],
            axis=2,
        )
        dma = pltpu.SemaphoreType.DMA
        any_spec = pl.BlockSpec(memory_space=pl.ANY)
        vmem_spec = pl.BlockSpec(memory_space=pltpu.VMEM)
        big, small = (2, 2, side * ROWS, half), (3, 2, ROWS, half)
        loss, dh, dw = pl.pallas_call(
            functools.partial(head_kernel, group, side, chunks, tokens),
            out_shape=(
                jax.ShapeDtypeStruct((1, 128), F32),
                jax.ShapeDtypeStruct((chunks, ROWS, dim), F32),
                jax.ShapeDtypeStruct((vocab, dim), F32),
            ),
            in_specs=[any_spec, vmem_spec, any_spec],
            out_specs=(vmem_spec, any_spec, any_spec),
            scratch_shapes=[
                pltpu.VMEM((2, vocab, dim), BF16),
                pltpu.VMEM((vocab, dim), F32),
                pltpu.VMEM((4, 2 * side, side, ROWS, dim), BF16),
                pltpu.VMEM((2, vocab, tok), F32),
                pltpu.VMEM((3, 2, vocab, tok // 2), BF16),
                pltpu.VMEM((2, vocab, tok // 2), BF16),
                pltpu.VMEM((2, side, side * ROWS, dim), F32),
                pltpu.VMEM((2, side, ROWS, dim), F32),
                *[pltpu.VMEM(big, F32)] * 3,
                *[pltpu.VMEM(small, F32)] * 3,
                pltpu.VMEM((2, ROWS, dim), F32),
                pltpu.VMEM((2, 2, tok), F32),
                pltpu.VMEM((2, 2, tok), F32),
                pltpu.VMEM((2, 2, tok), F32),
                pltpu.VMEM((2, 2, tok), F32),
                pltpu.VMEM((2, side, 2, tok), F32),
                pltpu.VMEM((2, 2, tok), F32),
                pltpu.VMEM((2, side, 2, tok), F32),
                pltpu.VMEM((1, tok), F32),
                pltpu.VMEM((1, tok), F32),
                dma((2,)), dma((4,)),
                dma((6, 3, 2)), dma((6, 3, 2)),
                dma, dma((2,)), dma, dma,
                dma((2,)), dma((2,)),
                dma((2, 2 * side - 1)), dma((2, side)),
                dma((2, 2 * side - 1)), dma((2, side)),
                dma((2,)), dma,
            ],
            compiler_params=pltpu.CompilerParams(
                collective_id=0, has_side_effects=True, vmem_limit_bytes=67043328,
            ),
            name="head",
        )(hid, tgt, w_blk)
        rows = tokens // group // 4
        pieces = (vocab + tokens // group) // rows
        dw, dh = pl.pallas_call(
            copy_kernel,
            out_shape=(jax.ShapeDtypeStruct((vocab, dim), F32), jax.ShapeDtypeStruct((tokens // group, dim), F32)),
            in_specs=[any_spec] * 2,
            out_specs=(any_spec, any_spec),
            scratch_shapes=[pltpu.VMEM((pieces, rows, dim), F32), dma((pieces,)), dma((pieces,))],
            compiler_params=pltpu.CompilerParams(vmem_limit_bytes=67043328),
            name="results",
        )(dw, dh.reshape(tokens // group, dim))
        return loss[0, :1], dh, dw

    return jax.shard_map(
        local_step,
        mesh=mesh,
        in_specs=(P("data", None), P("data"), P(AXIS, None)),
        out_specs=(P("data"), P(("data", AXIS), None), P(("data", AXIS), None)),
        check_vma=False,
    )
```

```python
import functools
import math

import jax
import jax.numpy as jnp
from jax import lax
from jax.experimental import pallas as pl
from jax.experimental.pallas import tpu as pltpu
from jax.sharding import PartitionSpec as P

F32 = jnp.float32
BF16 = jnp.bfloat16
LOG2E = 1.4426950408889634
LN2 = 0.6931471805599453
ROWS = 16
AXIS = "fsdp"

FAR1, PURE1, MERGED1, FAR2, PURE2, MERGED2 = range(6)


def dot_nt(a, b):
    return lax.dot_general(a, b, (((1,), (1,)), ((), ())), preferred_element_type=F32)


def dot_nn(a, b):
    return lax.dot_general(a, b, (((1,), (0,)), ((), ())), preferred_element_type=F32)


def dot_tn(a, b):
    return lax.dot_general(a, b, (((0,), (0,)), ((), ())), preferred_element_type=F32)


def join(parts):
    top = functools.reduce(jnp.maximum, parts)
    total = functools.reduce(jnp.add, [jnp.exp2(v - top) for v in parts])
    return top + jnp.log(total) * LOG2E


def head_kernel(
    group, side, chunks, tokens,
    hid, tgt, w_hbm,
    loss_ref, dh_hbm, dw_hbm,
    wb, dwacc, hb, yb, dz, dzr, sb, tb, far1, pure1, merged1, far2, pure2, merged2, ob,
    stat, own, st0, mid, st1, row, st2, lse, lossacc,
    wsem, hsem, rs_send, rs_recv, dz_send, dz_recv, w_send, w_recv,
    st0_send, st0_recv, st1_send, st1_recv, st2_send, st2_recv, osem, dwsem,
):
    vocab, dim = w_hbm.shape
    half = dim // 2
    mt = vocab // 2
    tok = hb.shape[1] * hb.shape[2] * ROWS
    tokc = tok // 2

    me = lax.axis_index(AXIS)
    core = lax.rem(me, 2)
    other = 1 - core
    x = lax.rem(me // 2, side)
    y = me // (2 * side)
    p = x + core * (y - x)
    q = y + core * (x - y)
    partner = me + 1 - 2 * core
    one = 1 + me // group

    def at_xy(xx, yy):
        return (lax.rem(yy + side, side) * side + lax.rem(xx + side, side)) * 2 + core

    def at_pq(pp, qq):
        return at_xy(pp + core * (qq - pp), qq + core * (pp - qq))

    peers_x = [at_xy(x + k, y) for k in range(1, side)]
    peers_y = [at_xy(x, y + k) for k in range(1, side)]
    to_p, to_q = (at_pq(p + 1, q), at_pq(p - 1, q)), (at_pq(p, q + 1), at_pq(p, q - 1))
    near_p = lax.rem(p + 1, side), lax.rem(p + side - 1, side), lax.rem(p + 2, side)
    near_q = lax.rem(q + 1, side), lax.rem(q + side - 1, side), lax.rem(q + 2, side)

    def rcopy(src, dst, send, recv, dev):
        return pltpu.make_async_remote_copy(
            src_ref=src, dst_ref=dst, send_sem=send, recv_sem=recv,
            device_id={AXIS: dev}, device_id_type=pl.DeviceIdType.MESH,
        )

    steady = [False]

    def guarded(cond, fn):
        if steady[0]:
            fn()
        else:
            pl.when(cond)(lambda: (fn(), None)[1])

    def both_ways(cond, fn):
        @pl.when(cond)
        def _():
            steady[0] = True
            fn()
            steady[0] = False

        pl.when(jnp.logical_not(cond))(fn)

    barrier = pltpu.get_barrier_semaphore()
    friends = [partner] + [peer + o for peer in (*peers_x, *peers_y) for o in (0, 1 - 2 * core)]
    for dev in friends:
        pl.semaphore_signal(barrier, inc=1, device_id={AXIS: dev}, device_id_type=pl.DeviceIdType.MESH)

    def h_copies(c):
        s = lax.rem(c, 4)
        out = []
        for k in range(side):
            out.append(pltpu.make_async_copy(hid.at[:, k, 0, c], hb.at[s, k], hsem.at[s]))
            out.append(pltpu.make_async_copy(hid.at[k, :, 1, c], hb.at[s, side + k], hsem.at[s]))
        return out

    def h_start(c):
        for d in h_copies(c):
            d.start()

    def h_wait(c):
        s = lax.rem(c, 4)
        pltpu.make_async_copy(hb.at[s], hb.at[s], hsem.at[s]).wait()

    w_local = pltpu.make_async_copy(w_hbm, wb.at[core], wsem)
    w_local.start()
    h_start(0)
    dwacc[...] = jnp.zeros_like(dwacc)
    lossacc[...] = jnp.zeros_like(lossacc)
    pl.semaphore_wait(barrier, len(friends))
    w_local.wait()
    w_remote = rcopy(wb.at[core], wb.at[core], w_send, w_recv, partner)
    w_remote.start()

    def rs(kind, c):
        s = t = lax.rem(c, 2)
        if kind >= FAR2:
            t = lax.rem(c, 3)
        lo, hi = pl.ds(0, half), pl.ds(half, half)
        buf, to, (up, down, far) = (sb, to_p, near_p) if kind < 3 else (tb, to_q, near_q)
        dst = (far1, pure1, merged1, far2, pure2, merged2)[kind]
        src = {0: ((far, lo), (far, hi)), 1: ((up, hi), (down, lo)), 2: ((up, lo), (down, hi))}[kind % 3]
        return [
            rcopy(buf.at[s, src[d][0], :, src[d][1]], dst.at[t, d], rs_send.at[kind, t, d], rs_recv.at[kind, t, d], to[d])
            for d in range(2)
        ]

    def start(ds):
        for d in ds:
            d.start()

    def wait_recv(ds):
        for d in ds:
            d.wait_recv()

    def wait_send(ds):
        for d in ds:
            d.wait_send()

    def dz_copy(c):
        s = lax.rem(c, 2)
        return [rcopy(dz.at[s, other], dzr.at[s], dz_send, dz_recv.at[s], partner)]

    def st0_copy(i):
        s = lax.rem(i, 2)
        return [rcopy(own.at[s], st0.at[s], st0_send.at[s], st0_recv.at[s], partner)]

    def st1_copy(i):
        s = lax.rem(i, 2)
        to = [(peer - o, k) for k, peer in enumerate(peers_x) for o in (0, 1)] + [(partner, side - 1)]
        return [rcopy(mid.at[s], st1.at[s, x], st1_send.at[s, n], st1_recv.at[s, k], dev) for n, (dev, k) in enumerate(to)]

    def st2_copy(i):
        s = lax.rem(i, 2)
        to = [(peer + o, k) for k, peer in enumerate(peers_y) for o in (0, 1)] + [(partner, side - 1)]
        return [rcopy(row.at[s], st2.at[s, y], st2_send.at[s, n], st2_recv.at[s, k], dev) for n, (dev, k) in enumerate(to)]

    def st_wait(copies, partner_core):
        wait_recv(copies[0:-1:2])
        pl.when(core == partner_core)(lambda: wait_recv(copies[-1:]))

    def two(fn):
        lax.fori_loop(0, 2, lambda j, carry: (fn(j), carry)[1], 0)

    def logits(i, j, slot):
        r = pl.ds(pl.multiple_of(j * mt, mt), mt)
        h = hb[lax.rem(i, 4)].reshape(tok, dim)
        yb[slot, r, :] = dot_nt(wb[core, r, :], h) * LOG2E

    def grad_logits(c, j, slot):
        r = pl.ds(pl.multiple_of(j * mt, mt), mt)
        prob = jnp.exp2(yb[slot, r, :] - lse[0:1, :]).astype(BF16)
        at_hit = (jnp.exp2(own[slot, 1:2, :] - lse[0:1, :]) - 1.0 / tokens).astype(BF16)
        rel = jnp.clip(tgt[c] - (me * vocab + j * mt), -1, mt).astype(jnp.int16)
        hit = lax.broadcasted_iota(jnp.int32, prob.shape, 0).astype(jnp.int16) == rel
        g = jnp.where(hit, at_hit, prob)
        dz[slot, 0, r, :] = g[:, :tokc]
        dz[slot, 1, r, :] = g[:, tokc:]

    def statistics(i, j, slot):
        v = yb[slot, pl.ds(pl.multiple_of(j * mt, mt), mt), :]
        top = jnp.max(v, axis=0, keepdims=True)
        total = jnp.sum(jnp.exp2(v - top), axis=0, keepdims=True)
        hit = lax.broadcasted_iota(jnp.int32, v.shape, 0) == tgt[lax.rem(i, chunks)] - (me * vocab + j * mt)
        stat[j, 0:1, :] = top + jnp.log(total) * LOG2E
        stat[j, 1:2, :] = jnp.sum(jnp.where(hit, v, 0.0), axis=0, keepdims=True)

    def grad_w(c, k):
        n = dim // 2
        cols = pl.ds(pl.multiple_of(k * n, n), n)
        h = hb[lax.rem(c, 4), :, :, :, cols].reshape(tok, n)
        s = lax.rem(c, 2)
        dwacc[:, cols] += dot_nn(dz[s, 0], h[:tokc]) + dot_nn(dz[s, 1], h[tokc:])

    def grad_h(c):
        s = lax.rem(c, 2)
        v = dot_tn(dz[s, core], wb[core]) + dot_tn(dzr[s], wb[other])
        sb[s] = v.reshape(side, side * ROWS, dim)

    def finish(c):
        s = lax.rem(c, 2)
        wait_recv(rs(PURE2, c) + rs(MERGED2, c))
        wait_send(rs(FAR2, c) + rs(PURE2, c) + rs(MERGED2, c))
        guarded(c >= 2, lambda: pltpu.make_async_copy(ob.at[s], dh_hbm.at[c - 2], osem.at[s]).wait())
        t = lax.rem(c, 3)
        ob[s, :, :half] = tb[s, q, :, :half] + merged2[t, 0] + pure2[t, 1]
        ob[s, :, half:] = tb[s, q, :, half:] + pure2[t, 0] + merged2[t, 1]
        pltpu.make_async_copy(ob.at[s], dh_hbm.at[c], osem.at[s]).start()

    def turn(c):
        s = lax.rem(c, 2)
        wait_recv(rs(PURE1, c) + rs(MERGED1, c))
        lo = sb[s, p, :, :half] + merged1[s, 0] + pure1[s, 1]
        hi = sb[s, p, :, half:] + pure1[s, 0] + merged1[s, 1]
        tb[s, :, :, :half] = lo.reshape(side, ROWS, half)
        tb[s, :, :, half:] = hi.reshape(side, ROWS, half)
        start(rs(FAR2, c) + rs(PURE2, c))
        wait_send(rs(FAR1, c) + rs(PURE1, c) + rs(MERGED1, c))

    def merge1(c):
        s = lax.rem(c, 2)
        up, down, _ = near_p
        wait_recv(rs(FAR1, c))
        sb[s, up, :, :half] += far1[s, 0]
        sb[s, down, :, half:] += far1[s, 1]
        start(rs(MERGED1, c))

    def merge2(c):
        s = lax.rem(c, 2)
        up, down, _ = near_q
        wait_recv(rs(FAR2, c))
        t = lax.rem(c, 3)
        tb[s, up, :, :half] += far2[t, 0]
        tb[s, down, :, half:] += far2[t, 1]
        start(rs(MERGED2, c))

    def st_own(i):
        s = lax.rem(i, 2)

        @pl.when(core == 0)
        def _():
            guarded(i >= 2, lambda: wait_send(st0_copy(i)))

        own[s, 0:1, :] = join([stat[0, 0:1, :], stat[1, 0:1, :]])
        own[s, 1:2, :] = stat[0, 1:2, :] + stat[1, 1:2, :]
        pl.when(core == 0)(lambda: start(st0_copy(i)))

    def st_pair(i):
        s = lax.rem(i, 2)

        @pl.when(core == 1)
        def _():
            wait_recv(st0_copy(i))
            guarded(i >= 2, lambda: wait_send(st1_copy(i)))
            mid[s, 0:1, :] = join([st0[s, 0:1, :], own[s, 0:1, :]])
            mid[s, 1:2, :] = st0[s, 1:2, :] + own[s, 1:2, :]
            start(st1_copy(i))

    def st_row(i):
        s = lax.rem(i, 2)
        st_wait(st1_copy(i), 0)

        @pl.when(core == 0)
        def _():
            guarded(i >= 2, lambda: wait_send(st2_copy(i)))
            row[s, 0:1, :] = join([st1[s, k, 0:1, :] for k in range(side)])
            row[s, 1:2, :] = functools.reduce(jnp.add, [st1[s, k, 1:2, :] for k in range(side)])
            st2[s, y] = row[s]
            start(st2_copy(i))

    def st_all(i):
        s = lax.rem(i, 2)
        st_wait(st2_copy(i), 1)
        full = join([st2[s, k, 0:1, :] for k in range(side)])
        hit = functools.reduce(jnp.add, [st2[s, k, 1:2, :] for k in range(side)])
        lse[0:1, :] = full + math.log2(tokens)
        lossacc[...] += full - hit

    def step(i, carry):
        c = i - 2
        slot = lax.rem(i, 2)
        has_a, has_c = i < chunks, jnp.logical_and(c >= 0, c < chunks)

        @pl.when(i + 1 < chunks)
        def _():
            h_start(i + 1)

        @pl.when(has_a)
        def _():
            h_wait(i)

        @pl.when(jnp.logical_and(has_a, has_c))
        def _():
            for j in range(2):
                grad_logits(c, j, slot)
                logits(i, j, slot)

        @pl.when(jnp.logical_and(has_a, jnp.logical_not(has_c)))
        def _():
            two(lambda j: logits(i, j, slot))
            two(lambda j: statistics(i, j, slot))

        @pl.when(jnp.logical_and(has_c, jnp.logical_not(has_a)))
        def _():
            two(lambda j: grad_logits(c, j, slot))

        def live(k):
            return jnp.logical_and(k >= 0, k < chunks)

        def live(k):
            return jnp.logical_and(k >= 0, k < chunks)

        calm = jnp.logical_and(i >= 7, i < chunks)

        def point_a():
            guarded(has_c, lambda: start(dz_copy(c)))
            guarded(live(c - 2), lambda: turn(c - 2))
            guarded(live(c - 1), lambda: start(rs(PURE1, c - 1)))

        def point_m():
            guarded(live(c - 1), lambda: merge1(c - 1))
            guarded(has_a, lambda: st_own(i))
            guarded(live(c - 3), lambda: finish(c - 3))

        def point_b():
            guarded(live(i - 1), lambda: st_all(i - 1))
            guarded(has_a, lambda: st_pair(i))
            guarded(has_c, lambda: (start(rs(FAR1, c)), wait_send(dz_copy(c))))
            guarded(live(c - 2), lambda: merge2(c - 2))

        both_ways(calm, point_a)

        now = jnp.logical_and(c >= 0, c < chunks - 2)

        @pl.when(now)
        def _():
            def half_dw(j):
                statistics(i, j, slot)
                grad_w(c, j)

            lax.fori_loop(0, one, lambda j, u: (half_dw(j), u)[1], 0)
            both_ways(calm, lambda: guarded(live(i - 1), lambda: st_row(i - 1)))
            lax.fori_loop(one, 2, lambda j, u: (half_dw(j), u)[1], 0)

        pl.when(jnp.logical_and(jnp.logical_not(now), live(i - 1)))(lambda: st_row(i - 1))

        @pl.when(c == chunks)
        def _():
            two(lambda j: grad_w(c - 2, j))

        both_ways(calm, point_m)

        @pl.when(has_c)
        def _():
            pl.when(c == 0)(w_remote.wait_recv)
            wait_recv(dz_copy(c))
            grad_h(c)

        both_ways(calm, point_b)

        @pl.when(c == chunks)
        def _():
            two(lambda j: grad_w(c - 1, j))
            pltpu.make_async_copy(dwacc, dw_hbm, dwsem).start()

        return carry

    lax.fori_loop(0, chunks + 5, step, 0)

    for i in range(max(chunks - 2, 0), chunks):
        guarded(core == 0, lambda: wait_send(st0_copy(i) + st2_copy(i)))
        guarded(core == 1, lambda: wait_send(st1_copy(i)))
        pltpu.make_async_copy(ob.at[i % 2], dh_hbm.at[i], osem.at[i % 2]).wait()
    w_remote.wait_send()
    pltpu.make_async_copy(dwacc, dw_hbm, dwsem).wait()
    loss_ref[...] = jnp.broadcast_to(jnp.sum(lossacc[...], axis=1, keepdims=True) * (LN2 / tokens), loss_ref.shape)


def copy_kernel(dw_hbm, dh_hbm, dw_out, dh_out, buf, isem, osem):
    rows = buf.shape[1]
    pieces = [(src.at[pl.ds(r, rows)], dst.at[pl.ds(r, rows)]) for src, dst in ((dw_hbm, dw_out), (dh_hbm, dh_out)) for r in range(0, src.shape[0], rows)]
    get = [pltpu.make_async_copy(src, buf.at[k], isem.at[k]) for k, (src, _) in enumerate(pieces)]
    put = [pltpu.make_async_copy(buf.at[k], dst, osem.at[k]) for k, (_, dst) in enumerate(pieces)]
    for copy in get:
        copy.start()
    for copy, back in zip(get, put):
        copy.wait()
        back.start()
    for back in put:
        back.wait()


def solution(mesh):
    group = mesh.shape[AXIS]
    side = math.isqrt(group // 2)

    def local_step(hidden, targets, w_blk):
        tokens, dim = hidden.shape
        vocab = w_blk.shape[0]
        chunks = tokens // group // ROWS
        tok = group * ROWS
        half = dim // 2
        hid = hidden.reshape(side, side, 2, chunks, ROWS, dim)
        t = targets.reshape(side, side, 2, chunks, ROWS)
        tgt = jnp.concatenate(
            [t[:, :, 0].transpose(2, 1, 0, 3).reshape(chunks, 1, tok // 2), t[:, :, 1].transpose(2, 0, 1, 3).reshape(chunks, 1, tok // 2)],
            axis=2,
        )
        dma = pltpu.SemaphoreType.DMA
        any_spec = pl.BlockSpec(memory_space=pl.ANY)
        vmem_spec = pl.BlockSpec(memory_space=pltpu.VMEM)
        big, small = (2, 2, side * ROWS, half), (3, 2, ROWS, half)
        loss, dh, dw = pl.pallas_call(
            functools.partial(head_kernel, group, side, chunks, tokens),
            out_shape=(
                jax.ShapeDtypeStruct((1, 128), F32),
                jax.ShapeDtypeStruct((chunks, ROWS, dim), F32),
                jax.ShapeDtypeStruct((vocab, dim), F32),
            ),
            in_specs=[any_spec, vmem_spec, any_spec],
            out_specs=(vmem_spec, any_spec, any_spec),
            scratch_shapes=[
                pltpu.VMEM((2, vocab, dim), BF16),
                pltpu.VMEM((vocab, dim), F32),
                pltpu.VMEM((4, 2 * side, side, ROWS, dim), BF16),
                pltpu.VMEM((2, vocab, tok), F32),
                pltpu.VMEM((2, 2, vocab, tok // 2), BF16),
                pltpu.VMEM((2, vocab, tok // 2), BF16),
                pltpu.VMEM((2, side, side * ROWS, dim), F32),
                pltpu.VMEM((2, side, ROWS, dim), F32),
                *[pltpu.VMEM(big, F32)] * 3,
                *[pltpu.VMEM(small, F32)] * 3,
                pltpu.VMEM((2, ROWS, dim), F32),
                pltpu.VMEM((2, 2, tok), F32),
                pltpu.VMEM((2, 2, tok), F32),
                pltpu.VMEM((2, 2, tok), F32),
                pltpu.VMEM((2, 2, tok), F32),
                pltpu.VMEM((2, side, 2, tok), F32),
                pltpu.VMEM((2, 2, tok), F32),
                pltpu.VMEM((2, side, 2, tok), F32),
                pltpu.VMEM((1, tok), F32),
                pltpu.VMEM((1, tok), F32),
                dma, dma((4,)),
                dma((6, 3, 2)), dma((6, 3, 2)),
                dma, dma((2,)), dma, dma,
                dma((2,)), dma((2,)),
                dma((2, 2 * side - 1)), dma((2, side)),
                dma((2, 2 * side - 1)), dma((2, side)),
                dma((2,)), dma,
            ],
            compiler_params=pltpu.CompilerParams(
                collective_id=0, has_side_effects=True, vmem_limit_bytes=67043328,
            ),
            name="head",
        )(hid, tgt, w_blk)
        rows = tokens // group // 4
        pieces = (vocab + tokens // group) // rows
        dw, dh = pl.pallas_call(
            copy_kernel,
            out_shape=(jax.ShapeDtypeStruct((vocab, dim), F32), jax.ShapeDtypeStruct((tokens // group, dim), F32)),
            in_specs=[any_spec] * 2,
            out_specs=(any_spec, any_spec),
            scratch_shapes=[pltpu.VMEM((pieces, rows, dim), F32), dma((pieces,)), dma((pieces,))],
            compiler_params=pltpu.CompilerParams(vmem_limit_bytes=67043328),
            name="results",
        )(dw, dh.reshape(tokens // group, dim))
        return loss[0, :1], dh, dw

    return jax.shard_map(
        local_step,
        mesh=mesh,
        in_specs=(P("data", None), P("data"), P(AXIS, None)),
        out_specs=(P("data"), P(("data", AXIS), None), P(("data", AXIS), None)),
        check_vma=False,
    )
```

```python
import functools
import math

import jax
import jax.numpy as jnp
from jax import lax
from jax.experimental import pallas as pl
from jax.experimental.pallas import tpu as pltpu
from jax.sharding import PartitionSpec as P

F32 = jnp.float32
BF16 = jnp.bfloat16
LOG2E = 1.4426950408889634
LN2 = 0.6931471805599453
ROWS = 16
AXIS = "fsdp"

FAR1, PURE1, MERGED1, FAR2, PURE2, MERGED2 = range(6)


def dot_nt(a, b):
    return lax.dot_general(a, b, (((1,), (1,)), ((), ())), preferred_element_type=F32)


def dot_nn(a, b):
    return lax.dot_general(a, b, (((1,), (0,)), ((), ())), preferred_element_type=F32)


def dot_tn(a, b):
    return lax.dot_general(a, b, (((0,), (0,)), ((), ())), preferred_element_type=F32)


def join(parts):
    top = functools.reduce(jnp.maximum, parts)
    total = functools.reduce(jnp.add, [jnp.exp2(v - top) for v in parts])
    return top + jnp.log(total) * LOG2E


def head_kernel(
    group, side, chunks, tokens,
    hid, tgt0, tgt1, w_hbm,
    loss_ref, dh_hbm, dw_hbm,
    wb, dwacc, hb, yb, dz, dzr, sb, tb, far1, pure1, merged1, far2, pure2, merged2, ob,
    stat, own, st0, mid, st1, row, st2, lse, lossacc,
    wsem, hsem, rs_send, rs_recv, dz_send, dz_recv, w_send, w_recv,
    st0_send, st0_recv, st1_send, st1_recv, st2_send, st2_recv, osem, dwsem,
):
    vocab, dim = w_hbm.shape
    half = dim // 2
    mt = vocab // 2
    tok = hb.shape[1] * hb.shape[2] * ROWS
    tokc = tok // 2

    me = lax.axis_index(AXIS)
    core = lax.rem(me, 2)
    other = 1 - core
    x = lax.rem(me // 2, side)
    y = me // (2 * side)
    p = x + core * (y - x)
    q = y + core * (x - y)
    partner = me + 1 - 2 * core
    one = 1 + me // group

    def at_xy(xx, yy):
        return (lax.rem(yy + side, side) * side + lax.rem(xx + side, side)) * 2 + core

    def at_pq(pp, qq):
        return at_xy(pp + core * (qq - pp), qq + core * (pp - qq))

    peers_x = [at_xy(x + k, y) for k in range(1, side)]
    peers_y = [at_xy(x, y + k) for k in range(1, side)]
    to_p, to_q = (at_pq(p + 1, q), at_pq(p - 1, q)), (at_pq(p, q + 1), at_pq(p, q - 1))
    near_p = lax.rem(p + 1, side), lax.rem(p + side - 1, side), lax.rem(p + 2, side)
    near_q = lax.rem(q + 1, side), lax.rem(q + side - 1, side), lax.rem(q + 2, side)

    def rcopy(src, dst, send, recv, dev):
        return pltpu.make_async_remote_copy(
            src_ref=src, dst_ref=dst, send_sem=send, recv_sem=recv,
            device_id={AXIS: dev}, device_id_type=pl.DeviceIdType.MESH,
        )

    steady = [False]

    def guarded(cond, fn):
        if steady[0]:
            fn()
        else:
            pl.when(cond)(lambda: (fn(), None)[1])

    def both_ways(cond, fn):
        @pl.when(cond)
        def _():
            steady[0] = True
            fn()
            steady[0] = False

        pl.when(jnp.logical_not(cond))(fn)

    barrier = pltpu.get_barrier_semaphore()
    friends = [partner] + [peer + o for peer in (*peers_x, *peers_y) for o in (0, 1 - 2 * core)]
    for dev in friends:
        pl.semaphore_signal(barrier, inc=1, device_id={AXIS: dev}, device_id_type=pl.DeviceIdType.MESH)

    def h_copies(c):
        s = lax.rem(c, 4)
        out = []
        for k in range(side):
            out.append(pltpu.make_async_copy(hid.at[:, k, 0, c], hb.at[s, k], hsem.at[s]))
            out.append(pltpu.make_async_copy(hid.at[k, :, 1, c], hb.at[s, side + k], hsem.at[s]))
        return out

    def h_start(c):
        for d in h_copies(c):
            d.start()

    def h_wait(c):
        s = lax.rem(c, 4)
        pltpu.make_async_copy(hb.at[s], hb.at[s], hsem.at[s]).wait()

    w_local = pltpu.make_async_copy(w_hbm, wb.at[core], wsem)
    w_local.start()
    h_start(0)
    dwacc[...] = jnp.zeros_like(dwacc)
    lossacc[...] = jnp.zeros_like(lossacc)
    pl.semaphore_wait(barrier, len(friends))
    w_local.wait()
    w_remote = rcopy(wb.at[core], wb.at[core], w_send, w_recv, partner)
    w_remote.start()

    def rs(kind, c):
        s = t = lax.rem(c, 2)
        if kind >= FAR2:
            t = lax.rem(c, 3)
        lo, hi = pl.ds(0, half), pl.ds(half, half)
        buf, to, (up, down, far) = (sb, to_p, near_p) if kind < 3 else (tb, to_q, near_q)
        dst = (far1, pure1, merged1, far2, pure2, merged2)[kind]
        src = {0: ((far, lo), (far, hi)), 1: ((up, hi), (down, lo)), 2: ((up, lo), (down, hi))}[kind % 3]
        return [
            rcopy(buf.at[s, src[d][0], :, src[d][1]], dst.at[t, d], rs_send.at[kind, t, d], rs_recv.at[kind, t, d], to[d])
            for d in range(2)
        ]

    def start(ds):
        for d in ds:
            d.start()

    def wait_recv(ds):
        for d in ds:
            d.wait_recv()

    def wait_send(ds):
        for d in ds:
            d.wait_send()

    def dz_copy(c):
        s = lax.rem(c, 2)
        return [rcopy(dz.at[s, other], dzr.at[s], dz_send, dz_recv.at[s], partner)]

    def st0_copy(i):
        s = lax.rem(i, 2)
        return [rcopy(own.at[s], st0.at[s], st0_send.at[s], st0_recv.at[s], partner)]

    def st1_copy(i):
        s = lax.rem(i, 2)
        to = [(peer - o, k) for k, peer in enumerate(peers_x) for o in (0, 1)] + [(partner, side - 1)]
        return [rcopy(mid.at[s], st1.at[s, x], st1_send.at[s, n], st1_recv.at[s, k], dev) for n, (dev, k) in enumerate(to)]

    def st2_copy(i):
        s = lax.rem(i, 2)
        to = [(peer + o, k) for k, peer in enumerate(peers_y) for o in (0, 1)] + [(partner, side - 1)]
        return [rcopy(row.at[s], st2.at[s, y], st2_send.at[s, n], st2_recv.at[s, k], dev) for n, (dev, k) in enumerate(to)]

    def st_wait(copies, partner_core):
        wait_recv(copies[0:-1:2])
        pl.when(core == partner_core)(lambda: wait_recv(copies[-1:]))

    def two(fn):
        lax.fori_loop(0, 2, lambda j, carry: (fn(j), carry)[1], 0)

    def targets(n):
        return jnp.concatenate([tgt0[n], tgt1[n]], axis=1)

    def logits(i, j, slot, mt=mt):
        r = pl.ds(pl.multiple_of(j * mt, mt), mt)
        h = hb[lax.rem(i, 4)].reshape(tok, dim)
        yb[slot, r, :] = dot_nt(wb[core, r, :], h) * LOG2E

    def grad_logits(c, j, slot, mt=mt):
        r = pl.ds(pl.multiple_of(j * mt, mt), mt)
        prob = jnp.exp2(yb[slot, r, :] - lse[0:1, :]).astype(BF16)
        at_hit = (jnp.exp2(own[slot, 1:2, :] - lse[0:1, :]) - 1.0 / tokens).astype(BF16)
        rel = jnp.clip(targets(c) - (me * vocab + j * mt), -1, mt).astype(jnp.int16)
        hit = lax.broadcasted_iota(jnp.int32, prob.shape, 0).astype(jnp.int16) == rel
        g = jnp.where(hit, at_hit, prob)
        dz[slot, 0, r, :] = g[:, :tokc]
        dz[slot, 1, r, :] = g[:, tokc:]

    def statistics(i, j, slot):
        v = yb[slot, pl.ds(pl.multiple_of(j * mt, mt), mt), :]
        top = jnp.max(v, axis=0, keepdims=True)
        total = jnp.sum(jnp.exp2(v - top), axis=0, keepdims=True)
        hit = lax.broadcasted_iota(jnp.int32, v.shape, 0) == targets(lax.rem(i, chunks)) - (me * vocab + j * mt)
        stat[j, 0:1, :] = top + jnp.log(total) * LOG2E
        stat[j, 1:2, :] = jnp.sum(jnp.where(hit, v, 0.0), axis=0, keepdims=True)

    def grad_w(c, k):
        n = dim // 2
        cols = pl.ds(pl.multiple_of(k * n, n), n)
        h = hb[lax.rem(c, 4), :, :, :, cols].reshape(tok, n)
        s = lax.rem(c, 2)
        dwacc[:, cols] += dot_nn(dz[s, 0], h[:tokc]) + dot_nn(dz[s, 1], h[tokc:])

    def grad_h(c):
        s = lax.rem(c, 2)
        v = dot_tn(dz[s, core], wb[core]) + dot_tn(dzr[s], wb[other])
        sb[s] = v.reshape(side, side * ROWS, dim)

    def finish(c):
        s = lax.rem(c, 2)
        wait_recv(rs(PURE2, c) + rs(MERGED2, c))
        wait_send(rs(FAR2, c) + rs(PURE2, c) + rs(MERGED2, c))
        guarded(c >= 2, lambda: pltpu.make_async_copy(ob.at[s], dh_hbm.at[c - 2], osem.at[s]).wait())
        t = lax.rem(c, 3)
        ob[s, :, :half] = tb[s, q, :, :half] + merged2[t, 0] + pure2[t, 1]
        ob[s, :, half:] = tb[s, q, :, half:] + pure2[t, 0] + merged2[t, 1]
        pltpu.make_async_copy(ob.at[s], dh_hbm.at[c], osem.at[s]).start()

    def turn(c):
        s = lax.rem(c, 2)
        wait_recv(rs(PURE1, c) + rs(MERGED1, c))
        lo = sb[s, p, :, :half] + merged1[s, 0] + pure1[s, 1]
        hi = sb[s, p, :, half:] + pure1[s, 0] + merged1[s, 1]
        tb[s, :, :, :half] = lo.reshape(side, ROWS, half)
        tb[s, :, :, half:] = hi.reshape(side, ROWS, half)
        wait_send(rs(FAR1, c) + rs(PURE1, c) + rs(MERGED1, c))

    def merge1(c):
        s = lax.rem(c, 2)
        up, down, _ = near_p
        wait_recv(rs(FAR1, c))
        sb[s, up, :, :half] += far1[s, 0]
        sb[s, down, :, half:] += far1[s, 1]
        start(rs(MERGED1, c))

    def merge2(c):
        s = lax.rem(c, 2)
        up, down, _ = near_q
        wait_recv(rs(FAR2, c))
        t = lax.rem(c, 3)
        tb[s, up, :, :half] += far2[t, 0]
        tb[s, down, :, half:] += far2[t, 1]
        start(rs(MERGED2, c))

    def st_own(i):
        s = lax.rem(i, 2)

        @pl.when(core == 0)
        def _():
            guarded(i >= 2, lambda: wait_send(st0_copy(i)))

        own[s, 0:1, :] = join([stat[0, 0:1, :], stat[1, 0:1, :]])
        own[s, 1:2, :] = stat[0, 1:2, :] + stat[1, 1:2, :]
        pl.when(core == 0)(lambda: start(st0_copy(i)))

    def st_pair(i):
        s = lax.rem(i, 2)

        @pl.when(core == 1)
        def _():
            wait_recv(st0_copy(i))
            guarded(i >= 2, lambda: wait_send(st1_copy(i)))
            mid[s, 0:1, :] = join([st0[s, 0:1, :], own[s, 0:1, :]])
            mid[s, 1:2, :] = st0[s, 1:2, :] + own[s, 1:2, :]
            start(st1_copy(i))

    def st_row(i):
        s = lax.rem(i, 2)
        st_wait(st1_copy(i), 0)

        @pl.when(core == 0)
        def _():
            guarded(i >= 2, lambda: wait_send(st2_copy(i)))
            row[s, 0:1, :] = join([st1[s, k, 0:1, :] for k in range(side)])
            row[s, 1:2, :] = functools.reduce(jnp.add, [st1[s, k, 1:2, :] for k in range(side)])
            st2[s, y] = row[s]
            start(st2_copy(i))

    def st_all(i):
        s = lax.rem(i, 2)
        st_wait(st2_copy(i), 1)
        full = join([st2[s, k, 0:1, :] for k in range(side)])
        hit = functools.reduce(jnp.add, [st2[s, k, 1:2, :] for k in range(side)])
        lse[0:1, :] = full + math.log2(tokens)
        lossacc[...] += full - hit

    def step(i, carry):
        c = i - 2
        slot = lax.rem(i, 2)
        has_a, has_c = i < chunks, jnp.logical_and(c >= 0, c < chunks)

        @pl.when(i + 1 < chunks)
        def _():
            h_start(i + 1)

        @pl.when(has_a)
        def _():
            h_wait(i)

        @pl.when(jnp.logical_and(has_a, has_c))
        def _():
            for j in range(4):
                grad_logits(c, j, slot, vocab // 4)
                logits(i, j, slot, vocab // 4)

        @pl.when(jnp.logical_and(has_a, jnp.logical_not(has_c)))
        def _():
            for j in range(2):
                logits(i, j, slot)
            for j in range(2):
                statistics(i, j, slot)

        @pl.when(jnp.logical_and(has_c, jnp.logical_not(has_a)))
        def _():
            two(lambda j: grad_logits(c, j, slot))

        def live(k):
            return jnp.logical_and(k >= 0, k < chunks)

        def live(k):
            return jnp.logical_and(k >= 0, k < chunks)

        calm = jnp.logical_and(i >= 7, i < chunks)

        def point_a():
            guarded(has_c, lambda: start(dz_copy(c)))
            guarded(live(c - 2), lambda: turn(c - 2))
            guarded(live(c - 1), lambda: start(rs(PURE1, c - 1)))

        def point_r():
            guarded(live(i - 1), lambda: st_row(i - 1))
            guarded(live(c - 2), lambda: start(rs(FAR2, c - 2) + rs(PURE2, c - 2)))

        def point_m():
            guarded(live(c - 1), lambda: merge1(c - 1))
            guarded(has_a, lambda: st_own(i))
            guarded(live(c - 3), lambda: finish(c - 3))

        def point_b():
            guarded(live(i - 1), lambda: st_all(i - 1))
            guarded(has_a, lambda: st_pair(i))
            guarded(has_c, lambda: (start(rs(FAR1, c)), wait_send(dz_copy(c))))
            guarded(live(c - 2), lambda: merge2(c - 2))

        both_ways(calm, point_a)

        now = jnp.logical_and(c >= 0, c < chunks - 2)

        @pl.when(now)
        def _():
            def half_dw(j):
                statistics(i, j, slot)
                grad_w(c, j)

            lax.fori_loop(0, one, lambda j, u: (half_dw(j), u)[1], 0)
            both_ways(calm, point_r)
            lax.fori_loop(one, 2, lambda j, u: (half_dw(j), u)[1], 0)

        pl.when(jnp.logical_not(now))(point_r)

        @pl.when(c == chunks)
        def _():
            two(lambda j: grad_w(c - 2, j))

        both_ways(calm, point_m)

        @pl.when(has_c)
        def _():
            pl.when(c == 0)(w_remote.wait_recv)
            wait_recv(dz_copy(c))
            grad_h(c)

        both_ways(calm, point_b)

        @pl.when(c == chunks)
        def _():
            two(lambda j: grad_w(c - 1, j))
            pltpu.make_async_copy(dwacc, dw_hbm, dwsem).start()

        return carry

    lax.fori_loop(0, chunks + 5, step, 0)

    for i in range(max(chunks - 2, 0), chunks):
        guarded(core == 0, lambda: wait_send(st0_copy(i) + st2_copy(i)))
        guarded(core == 1, lambda: wait_send(st1_copy(i)))
        pltpu.make_async_copy(ob.at[i % 2], dh_hbm.at[i], osem.at[i % 2]).wait()
    w_remote.wait_send()
    pltpu.make_async_copy(dwacc, dw_hbm, dwsem).wait()
    loss_ref[...] = jnp.broadcast_to(jnp.sum(lossacc[...], axis=1, keepdims=True) * (LN2 / tokens), loss_ref.shape)


def copy_kernel(dw_hbm, dh_hbm, dw_out, dh_out, buf, isem, osem):
    rows = buf.shape[1]
    pieces = [(src.at[pl.ds(r, rows)], dst.at[pl.ds(r, rows)]) for src, dst in ((dw_hbm, dw_out), (dh_hbm, dh_out)) for r in range(0, src.shape[0], rows)]
    get = [pltpu.make_async_copy(src, buf.at[k], isem.at[k]) for k, (src, _) in enumerate(pieces)]
    put = [pltpu.make_async_copy(buf.at[k], dst, osem.at[k]) for k, (_, dst) in enumerate(pieces)]
    for copy in get:
        copy.start()
    for copy, back in zip(get, put):
        copy.wait()
        back.start()
    for back in put:
        back.wait()


def solution(mesh):
    group = mesh.shape[AXIS]
    side = math.isqrt(group // 2)

    def local_step(hidden, targets, w_blk):
        tokens, dim = hidden.shape
        vocab = w_blk.shape[0]
        chunks = tokens // group // ROWS
        tok = group * ROWS
        half = dim // 2
        hid = hidden.reshape(side, side, 2, chunks, ROWS, dim)
        t = targets.reshape(side, side, 2, chunks, ROWS)
        tgt0 = t[:, :, 0].transpose(2, 1, 0, 3).reshape(chunks, 1, tok // 2)
        tgt1 = t[:, :, 1].transpose(2, 0, 1, 3).reshape(chunks, 1, tok // 2)
        dma = pltpu.SemaphoreType.DMA
        any_spec = pl.BlockSpec(memory_space=pl.ANY)
        vmem_spec = pl.BlockSpec(memory_space=pltpu.VMEM)
        big, small = (2, 2, side * ROWS, half), (3, 2, ROWS, half)
        loss, dh, dw = pl.pallas_call(
            functools.partial(head_kernel, group, side, chunks, tokens),
            out_shape=(
                jax.ShapeDtypeStruct((1, 128), F32),
                jax.ShapeDtypeStruct((chunks, ROWS, dim), F32),
                jax.ShapeDtypeStruct((vocab, dim), F32),
            ),
            in_specs=[any_spec, vmem_spec, vmem_spec, any_spec],
            out_specs=(vmem_spec, any_spec, any_spec),
            scratch_shapes=[
                pltpu.VMEM((2, vocab, dim), BF16),
                pltpu.VMEM((vocab, dim), F32),
                pltpu.VMEM((4, 2 * side, side, ROWS, dim), BF16),
                pltpu.VMEM((2, vocab, tok), F32),
                pltpu.VMEM((2, 2, vocab, tok // 2), BF16),
                pltpu.VMEM((2, vocab, tok // 2), BF16),
                pltpu.VMEM((2, side, side * ROWS, dim), F32),
                pltpu.VMEM((2, side, ROWS, dim), F32),
                *[pltpu.VMEM(big, F32)] * 3,
                *[pltpu.VMEM(small, F32)] * 3,
                pltpu.VMEM((2, ROWS, dim), F32),
                pltpu.VMEM((2, 2, tok), F32),
                pltpu.VMEM((2, 2, tok), F32),
                pltpu.VMEM((2, 2, tok), F32),
                pltpu.VMEM((2, 2, tok), F32),
                pltpu.VMEM((2, side, 2, tok), F32),
                pltpu.VMEM((2, 2, tok), F32),
                pltpu.VMEM((2, side, 2, tok), F32),
                pltpu.VMEM((1, tok), F32),
                pltpu.VMEM((1, tok), F32),
                dma, dma((4,)),
                dma((6, 3, 2)), dma((6, 3, 2)),
                dma, dma((2,)), dma, dma,
                dma((2,)), dma((2,)),
                dma((2, 2 * side - 1)), dma((2, side)),
                dma((2, 2 * side - 1)), dma((2, side)),
                dma((2,)), dma,
            ],
            compiler_params=pltpu.CompilerParams(
                collective_id=0, has_side_effects=True, vmem_limit_bytes=67043328,
            ),
            name="head",
        )(hid, tgt0, tgt1, w_blk)
        rows = tokens // group // 4
        pieces = (vocab + tokens // group) // rows
        dw, dh = pl.pallas_call(
            copy_kernel,
            out_shape=(jax.ShapeDtypeStruct((vocab, dim), F32), jax.ShapeDtypeStruct((tokens // group, dim), F32)),
            in_specs=[any_spec] * 2,
            out_specs=(any_spec, any_spec),
            scratch_shapes=[pltpu.VMEM((pieces, rows, dim), F32), dma((pieces,)), dma((pieces,))],
            compiler_params=pltpu.CompilerParams(vmem_limit_bytes=67043328),
            name="results",
        )(dw, dh.reshape(tokens // group, dim))
        return loss[0, :1], dh, dw

    return jax.shard_map(
        local_step,
        mesh=mesh,
        in_specs=(P("data", None), P("data"), P(AXIS, None)),
        out_specs=(P("data"), P(("data", AXIS), None), P(("data", AXIS), None)),
        check_vma=False,
    )
```
